32 devices in a mesh: groups: 2 (over y), expert: 4 (over z), tensor: 4 (over x, core).
Axes of the slice: x: 2, y: 2, z: 4, core: 2. Of those that a mesh axis runs over, the one named last changes fastest.
Arguments:
- kv_prefill: bfloat16 [32, 512, 2, 1024], P('groups', 'expert', None, 'tensor'), parts along dimension 0, may hold values from -8 to 8
- slot_of: int32 [32], P('groups'), parts along dimension 0, may hold values from 0 to 15, as said below
- lengths: int32 [32], P('groups'), parts along dimension 0, may hold values from 2 to 512
- query: bfloat16 [32, 4096], P(('groups', 'expert'), 'tensor'), parts along dimension 0, may hold values from -100 to 100
- new_kv: bfloat16 [32, 2, 1024], P(('groups', 'expert'), None, 'tensor'), parts along dimension 0, may hold values from -6 to 6
- wo: bfloat16 [4096, 4096], P('tensor', 'expert'), may hold values from -0.09375 to 0.09375
- resid: bfloat16 [32, 4096], P('groups', 'expert'), parts along dimension 0, may hold values from -60 to 60
- norm_gain: bfloat16 [4096], P('expert'), may hold values from 0.25 to 1.75
- expert_ids: int32 [32, 2], P('groups'), parts along dimension 0, may hold values from 0 to 3, all different within a row; in each aligned block of 16 rows (0 to 15, 16 to 31, ...) at most 12 rows name the same one
- gate_logits: float32 [32, 2], P('groups'), parts along dimension 0, may hold values from -6 to 6
- gate_weight_slabs: bfloat16 [4, 4096, 8192], P('expert', None, 'tensor'), may hold values from -0.09375 to 0.09375
- w_up: bfloat16 [4, 4096, 8192], P('expert', None, 'tensor'), may hold values from -0.09375 to 0.09375
- w_down: bfloat16 [4, 8192, 4096], P('expert', 'tensor'), may hold values from -0.0625 to 0.0625
Outputs:
- attn_out: bfloat16 [32, 4096], P('groups', 'expert'), parts along dimension 0
- moe_out: bfloat16 [32, 4096], P(('groups', 'tensor'), 'expert'), parts along dimension 0
The draws below stay inside these ranges and needn't reach their ends.
There are 2 independent parts, one for each index of `groups`. The reference program is written for one: setup_inputs(seed, part) draws one part's arguments, and reference() takes and returns one part's arrays. A program takes and returns all parts, laid end to end along the dimension named above; an argument that names none is the same for every part. Nothing has to cross between parts.
Inputs may be any that keep to these rules, and one draw needn't show every extreme that they name: `slot_of`: a permutation of 0 to 15. `expert_ids`: each expert is named by at most 12 tokens, one of them by exactly 12; no token names an expert twice.
All inputs are finite; a program needn't handle non-finite values.
Results may differ from the reference program's by a relative error of at most 0.023.
Values may be sent and summed in bfloat16 or wider, within the bound.
No kernel may reach another device: no remote copies, remote signals or barrier semaphores. Data moves between devices by JAX's collectives and lax.ppermute only.
A program may use at most 128 MiB of HBM per device.

```python
import math
import jax
import jax.numpy as jnp
import numpy as np
from jax import lax

D = 4096
HEADS = 32
KVH = 8
HD = 128
FF = 8192
EXPERTS = 4
TOPK = 2
L = 512
B = 16
SUB = 1
CAP = 12


def slot_order(key):
    return jax.random.permutation(jax.random.fold_in(key, 11), B).astype(jnp.int32)


def draw_slot_of(key, part):
    return slot_order(key)


def draw_kv_prefill(key, part):
    shape_all = (B, L, 2, KVH * HD)
    drawn = jnp.clip(jax.random.normal(jax.random.fold_in(key, 21), shape_all, jnp.float32), -6.0, 6.0)
    return drawn.astype(jnp.bfloat16)


def draw_query(key, part):
    shape_all = (B, HEADS * HD)
    drawn = jnp.clip(jax.random.normal(jax.random.fold_in(key, 41), shape_all, jnp.float32), -6.0, 6.0)
    return drawn.astype(jnp.bfloat16)


def draw_resid(key, part):
    column = jnp.arange(D, dtype=jnp.float32) / D
    base_rows = jnp.clip(jax.random.normal(jax.random.fold_in(key, 53), (B, D), jnp.float32), -6.0, 6.0)
    column_scale = 0.3 * jnp.power(10.0, column)
    row_scale = jnp.exp(jax.random.uniform(jax.random.fold_in(key, 51), (B, 1), jnp.float32, math.log(0.3), math.log(3.0)))
    return (base_rows * row_scale * column_scale[None, :]).astype(jnp.bfloat16)


def place_ends(values, own_key, least, high):
    index_at = [jax.random.randint(jax.random.fold_in(own_key, axis), (), 0, length) for axis, length in enumerate(values.shape)]
    main_axis = values.shape.index(max(values.shape))
    next_to = index_at[:main_axis] + [(index_at[main_axis] + 1) % values.shape[main_axis]] + index_at[main_axis + 1:]
    return values.at[tuple(index_at)].set(least).at[tuple(next_to)].set(high)


def shard_levels(stream_key, shape, cuts, low, high):
    def one(position, parts):
        steps = jax.random.uniform(jax.random.fold_in(jax.random.fold_in(stream_key, 6), position), (parts,), jnp.float32, low / len(cuts), high / len(cuts))
        return jnp.repeat(jnp.exp(steps), shape[position] // parts).reshape((-1,) + (1,) * (len(shape) - position - 1))

    level = one(*cuts[0])
    for cut in cuts[1:]:
        level = level * one(*cut)
    return level


def assign_block(own_key, own, number, rows, amount, top, bound, lean):
    sequence = jax.random.permutation(own_key, amount)
    heavy_load, usual = portions_of(amount, rows * top, bound, lean, True), portions_of(amount, rows * top, bound, lean, False)
    places = jnp.arange(amount)

    def named(tallies, rotation):
        used = int((tallies > 0).sum())
        fixed = max(1, used // 4)
        moved = fixed + (places - fixed + rotation * (used - fixed)) % max(1, amount - fixed)
        return jnp.zeros((amount,), jnp.int32).at[sequence[jnp.where(places < fixed, places, moved)]].set(jnp.asarray(tallies, jnp.int32))

    tallies = jnp.where(number % 4 == 0, named(heavy_load, number // 4), named(usual, number - number // 4 - 1))
    mixed = jax.random.permutation(jax.random.fold_in(own, 3), amount)
    giver, receiver = mixed[0:amount // 2 * 2:2], mixed[1:amount // 2 * 2:2]
    room = jnp.minimum(tallies[giver] - 1, bound - tallies[receiver]) // 2
    room = jnp.where((giver == sequence[0]) | (receiver == sequence[0]) | (tallies[receiver] == 0), 0, jnp.maximum(room, 0))
    moved = jax.random.randint(jax.random.fold_in(own, 4), (amount // 2,), 0, 1 << 20) % (room + 1)
    tallies = tallies.at[giver].add(-moved).at[receiver].add(moved)
    items = jnp.searchsorted(jnp.cumsum(tallies), jnp.arange(rows * top), side="right").astype(jnp.int32)
    grid = items.reshape(top, rows).T
    grid = grid[jax.random.permutation(jax.random.fold_in(own, 1), rows)]
    rotation = jax.random.randint(jax.random.fold_in(own, 2), (rows, 1), 0, top)
    return jnp.take_along_axis(grid, (jnp.arange(top)[None, :] + rotation) % top, axis=1)


def portions_of(count, total, limit, skew, full):
    weights = [(1 << 20) // math.isqrt(grade ** skew) + 1 for grade in range(1, count + 1)]
    largest = limit if full else min(limit, max(-(-total // count), total * weights[0] // sum(weights)))
    least = 1 if total - largest >= count - 1 else 0
    holding, spare = [largest] + [least] * (count - 1), total - largest - least * (count - 1)
    while spare > 0:
        movable = [i for i in range(1, count) if holding[i] < largest] or [i for i in range(1, count) if holding[i] < limit]
        whole, remaining = sum([weights[i] for i in movable]), spare
        for i in movable:
            more = min(limit - holding[i], max(1, remaining * weights[i] // whole), spare)
            holding[i] = holding[i] + more
            spare = spare - more
    return np.array(holding)


def scatter_about(own_key, extent, spread, most, cuts=(), kind=jnp.bfloat16):
    loudness = shard_levels(own_key, extent, cuts, -0.22, 0.18) if cuts else 1.0
    values = jax.random.normal(own_key, extent, jnp.float32) * spread * loudness
    return jnp.minimum(jnp.maximum(values, -most), most).astype(kind)


def setup_inputs(seed: int = 0, part: int = 0) -> dict:
    key_list = jax.random.split(jax.random.key(seed), 14)
    own_keys = jax.random.split(jax.random.fold_in(key_list[13], part), 14)
    kv_prefill = draw_kv_prefill(jax.random.fold_in(jax.random.fold_in(key_list[13], part), 71), part)
    slot_of = draw_slot_of(jax.random.fold_in(jax.random.fold_in(key_list[13], part), 71), part)
    lengths = place_ends(jax.random.randint(own_keys[2], (B,), 2, L + 1), jax.random.fold_in(own_keys[2], 1), 2, L).astype(jnp.int32)
    query = draw_query(jax.random.fold_in(jax.random.fold_in(key_list[13], part), 71), part)
    new_kv = scatter_about(own_keys[4], (B, 2, KVH * HD), 1.0, 6.0, ((0, 4), (2, 4)))
    wo = scatter_about(key_list[5], (HEADS * HD, D), (HEADS * HD) ** -0.5, 0.09375, ((0, 4), (1, 4)))
    resid = draw_resid(jax.random.fold_in(jax.random.fold_in(key_list[13], part), 71), part)
    norm_gain = jnp.clip(1.0 + 0.15 * jax.random.normal(key_list[7], (D,), jnp.float32), 0.25, 1.75).astype(jnp.bfloat16)
    expert_ids_keys = jax.random.split(jax.random.fold_in(own_keys[8], 1), B // B)
    expert_ids_turns = jax.random.permutation(jax.random.fold_in(own_keys[8], 3), B // B)
    expert_ids = jax.vmap(lambda own, number: assign_block(jax.random.fold_in(own_keys[8], 2), own, number, B, EXPERTS, TOPK, CAP, 2))(expert_ids_keys, expert_ids_turns).reshape((B, TOPK))
    gate_logits = scatter_about(own_keys[9], (B, TOPK), 1.5, 6.0, (), jnp.float32)
    gate_weight_slabs = scatter_about(key_list[10], (EXPERTS * SUB, D, FF // SUB), D ** -0.5, 0.09375, ((0, 4), (2, 4)))
    w_up = scatter_about(key_list[11], (EXPERTS * SUB, D, FF // SUB), D ** -0.5, 0.09375, ((0, 4), (2, 4)))
    w_down = scatter_about(key_list[12], (EXPERTS * SUB, FF // SUB, D), FF ** -0.5, 0.0625, ((0, 4), (1, 4)))
    return {"kv_prefill": kv_prefill, "slot_of": slot_of, "lengths": lengths, "query": query, "new_kv": new_kv, "wo": wo, "resid": resid, "norm_gain": norm_gain, "expert_ids": expert_ids, "gate_logits": gate_logits, "gate_weight_slabs": gate_weight_slabs, "w_up": w_up, "w_down": w_down}


EPSILON = 1e-05

def reference(kv_prefill, slot_of, lengths, query, new_kv, wo, resid, norm_gain, expert_ids, gate_logits, gate_weight_slabs, w_up, w_down):
    group_size = HEADS // KVH
    logit_scale_factor = 1.0 / math.sqrt(HD)
    cached = jnp.take(kv_prefill, slot_of, axis=0)
    key_rows = cached[:, :, 0, :].reshape(B, L, KVH, HD).astype(jnp.float32)
    value_rows = cached[:, :, 1, :].reshape(B, L, KVH, HD).astype(jnp.float32)
    query_vectors = query.reshape(B, KVH, group_size, HD).astype(jnp.float32)
    scores = jnp.einsum('bkqd,bpkd->bkqp', query_vectors, key_rows) * logit_scale_factor
    live_mask = jnp.arange(L, dtype=jnp.int32)[None, :] < lengths[:, None]
    live_mask = live_mask[:, None, None, :]
    scores = jnp.where(live_mask, scores, -1e+30)
    cache_peak = lax.optimization_barrier(jnp.max(scores, axis=-1))
    exp_weights = jnp.where(live_mask, jnp.exp(scores - cache_peak[..., None]), 0.0)
    cache_total = lax.optimization_barrier(jnp.sum(exp_weights, axis=-1))
    rounded = lax.optimization_barrier(exp_weights.astype(jnp.bfloat16)).astype(jnp.float32)
    summed = jnp.einsum('bkqp,bpkd->bkqd', rounded, value_rows)
    fresh_key_rows = new_kv[:, 0, :].reshape(B, KVH, HD).astype(jnp.float32)
    new_values = new_kv[:, 1, :].reshape(B, KVH, HD).astype(jnp.float32)
    self_score_value = jnp.einsum('utfa,uta->utf', query_vectors, fresh_key_rows) * logit_scale_factor
    peak_value = jnp.maximum(cache_peak, self_score_value)
    old_part = jnp.exp(cache_peak - peak_value)
    own_part = jnp.exp(self_score_value - peak_value)
    numerator = summed * old_part[..., None] + own_part[..., None] * new_values[:, :, None, :]
    denominator = cache_total * old_part + own_part
    context = (numerator / denominator[..., None]).reshape(B, HEADS * HD).astype(jnp.bfloat16)
    attn_out = jnp.dot(context, wo, preferred_element_type=jnp.float32).astype(jnp.bfloat16)
    hidden_activation = resid.astype(jnp.float32) + attn_out.astype(jnp.float32)
    mean_square = lax.optimization_barrier(jnp.mean(hidden_activation * hidden_activation, axis=1, keepdims=True))
    normed = (hidden_activation * lax.rsqrt(mean_square + EPSILON) * norm_gain.astype(jnp.float32)[None, :]).astype(jnp.bfloat16)
    first_share = 1.0 / (1.0 + jnp.exp(gate_logits[:, 1] - gate_logits[:, 0]))
    shares = jnp.stack([first_share, 1.0 - first_share], axis=1)
    chosen = expert_ids[:, :, None] == jnp.arange(EXPERTS, dtype=jnp.int32)[None, None, :]
    mixture = lax.optimization_barrier(jnp.sum(jnp.where(chosen, shares[:, :, None], 0.0), axis=1))

    def expert_term(expert_index):
        slab_begin_offset = expert_index * SUB
        gate_slab = lax.dynamic_slice_in_dim(gate_weight_slabs, slab_begin_offset, SUB, 0)
        gate_slab = jnp.moveaxis(gate_slab, 0, 1).reshape(D, FF)
        up_slab = lax.dynamic_slice_in_dim(w_up, slab_begin_offset, SUB, 0)
        up_slab = jnp.moveaxis(up_slab, 0, 1).reshape(D, FF)
        down_slab = lax.dynamic_slice_in_dim(w_down, slab_begin_offset, SUB, 0).reshape(FF, D)
        gate_sum = jnp.dot(normed, gate_slab, preferred_element_type=jnp.float32)
        up_sum = jnp.dot(normed, up_slab, preferred_element_type=jnp.float32)
        activated = (jax.nn.silu(gate_sum) * up_sum).astype(jnp.bfloat16)
        weight_column = lax.dynamic_index_in_dim(mixture, expert_index, 1, keepdims=True)
        return jnp.dot(activated, down_slab, preferred_element_type=jnp.float32) * weight_column
    contributions = lax.map(expert_term, jnp.arange(EXPERTS, dtype=jnp.int32))
    moe_out = lax.optimization_barrier(jnp.sum(contributions, axis=0)).astype(jnp.bfloat16)
    return (attn_out, moe_out)
```

```python
import functools
import math

import jax
import jax.numpy as jnp
from jax import lax
from jax.experimental import pallas as pl
from jax.experimental.pallas import tpu as pltpu
from jax.sharding import PartitionSpec as P

HEADS = 32
KVH = 8
HD = 128
EXPERTS = 4
EPSILON = 1e-05
MASKED = -1e30
LIVE = -1e29
LANES = 128
STATS = 16
MOST_PERMUTES = 4

BF = jnp.bfloat16
F32 = jnp.float32
VMEM = pl.BlockSpec(memory_space=pltpu.VMEM)
SMEM = pl.BlockSpec(memory_space=pltpu.SMEM)
HBM = pl.BlockSpec(memory_space=pltpu.HBM)


def gather(value, axis):
    count = lax.axis_size(axis)
    if count > MOST_PERMUTES:
        return [lax.all_gather(value, axis)]
    out = [value]
    for shift in range(1, count):
        out.append(lax.ppermute(value, axis, [(i, (i + shift) % count) for i in range(count)]))
    return out


def exchange(values, axis):
    count = lax.axis_size(axis)
    if count > MOST_PERMUTES:
        return [lax.all_to_all(values[0], axis, 0, 0, tiled=True)]
    out = [values[0]]
    for shift in range(1, count):
        out.append(
            lax.ppermute(values[shift], axis, [(i, (i + shift) % count) for i in range(count)])
        )
    return out


def piece(refs, count, shift):
    return refs[shift][...] if len(refs) == count else refs[0][shift]


def source(refs, count, me, shift):
    return lax.rem(me - shift + count, count) if len(refs) == count else shift


def target(stacked, count, me, shift):
    return shift if stacked else lax.rem(me + shift, count)


def grouped(count):
    return 1 if count > MOST_PERMUTES else count


def attend_kernel(count, own_rows, kv_heads, group, positions, *refs):
    taken = grouped(count)
    slot_ref, length_ref = refs[0], refs[1]
    query_refs = refs[2 : 2 + taken]
    new_ref, cache_ref, out_ref = refs[2 + taken : 5 + taken]
    q_rows, score, acc, fresh = refs[5 + taken :]
    me = lax.axis_index("expert")
    heads = kv_heads * group
    total = count * own_rows
    rows = total * heads
    width = 2 * positions
    scale = 1.0 / math.sqrt(HD)
    for shift in range(count):
        block = piece(query_refs, count, shift).astype(F32)
        where_to = source(query_refs, count, me, shift)
        for head in range(heads):
            q_rows[where_to, pl.ds(head, own_rows, stride=heads), :] = block[
                :, head * HD : (head + 1) * HD
            ]
    head_of_row = lax.broadcasted_iota(jnp.int32, (heads, HD), 0) // group
    lane = lax.broadcasted_iota(jnp.int32, (heads, width), 1)
    position = me * positions + lane // 2
    is_key = lax.rem(lane, 2) == 0

    def diagonal(parts):
        return sum(jnp.where(head_of_row == g, parts(g), 0.0) for g in range(kv_heads))

    def scores(b):
        owner, within = b // own_rows, lax.rem(b, own_rows)
        vectors = q_rows[owner, pl.ds(pl.multiple_of(within * heads, heads), heads), :]
        spread = jnp.concatenate(
            [jnp.where(head_of_row == g, vectors, 0.0) for g in range(kv_heads)], axis=1
        ).astype(BF)
        both = cache_ref[slot_ref[b]]
        found = (
            lax.dot_general(
                spread, both, (((1,), (1,)), ((), ())), preferred_element_type=F32
            )
            * scale
        )
        live = is_key & (position < length_ref[b])
        score[pl.ds(pl.multiple_of(b * heads, heads), heads), :] = jnp.where(live, found, MASKED)

    def values(b):
        at = pl.ds(pl.multiple_of(b * heads, heads), heads)
        both = cache_ref[slot_ref[b]]
        summed = jnp.dot(score[at, :].astype(BF), both, preferred_element_type=F32)
        acc[at, :] = diagonal(lambda g: summed[:, g * HD : (g + 1) * HD])

    def sweep(step):
        if total <= 16:
            for b in range(total):
                step(b)
        else:
            pl.loop(0, total)(step)

    sweep(scores)
    own = own_rows * heads
    new = new_ref[...].astype(F32)
    for b in range(own_rows):
        for g in range(kv_heads):
            at = b * heads + g * group
            for which in range(2):
                fresh[which, at : at + group, :] = jnp.broadcast_to(
                    new[b, which : which + 1, g * HD : (g + 1) * HD], (group, HD)
                )
    own_score = jnp.sum(q_rows[me] * fresh[0], axis=1, keepdims=True) * scale
    row = lax.broadcasted_iota(jnp.int32, (rows, 1), 0)
    at_home = (row >= me * own) & (row < (me + 1) * own)
    own_all = jnp.concatenate([own_score] * count, axis=0)
    own_all = jnp.where(at_home, own_all, MASKED)
    raw = score[...]
    peak = jnp.maximum(jnp.max(raw, axis=1, keepdims=True), own_all).astype(BF).astype(F32)
    weights = jnp.where(raw > LIVE, jnp.exp(raw - peak), 0.0)
    own_weight = jnp.where(at_home, jnp.exp(own_all - peak), 0.0)
    weight_sum = jnp.sum(weights, axis=1, keepdims=True) + own_weight
    score[...] = pltpu.roll(weights, 1, 1)
    sweep(values)
    fresh_all = jnp.concatenate([fresh[1]] * count, axis=0)
    out_ref[0:rows, :] = (acc[...] + own_weight * fresh_all).astype(BF)
    high = weight_sum.astype(BF).astype(F32)
    low = weight_sum - high
    column = lax.broadcasted_iota(jnp.int32, (rows, LANES), 1)
    table = jnp.where(
        column == 0, peak, jnp.where(column == 1, high, jnp.where(column == 2, low, 0.0))
    )
    for part in range(rows // LANES):
        turned = table[part * LANES : (part + 1) * LANES, :].T
        out_ref[rows + part * STATS : rows + (part + 1) * STATS, :] = turned[0:STATS, :].astype(BF)


def attend(slot_of, lengths, queries, new_kv, cache, count):
    own_rows, _, kv_width = new_kv.shape
    kv_heads = kv_width // HD
    group = HEADS // KVH
    heads = kv_heads * group
    positions = cache.shape[1] // 2
    rows = count * own_rows * heads
    return pl.pallas_call(
        functools.partial(attend_kernel, count, own_rows, kv_heads, group, positions),
        name="attend",
        out_shape=jax.ShapeDtypeStruct((rows + STATS * (rows // LANES), LANES), BF),
        in_specs=[SMEM, SMEM] + [VMEM] * (len(queries) + 2),
        out_specs=VMEM,
        scratch_shapes=[
            pltpu.VMEM((count, own_rows * heads, HD), F32),
            pltpu.VMEM((rows, 2 * positions), F32),
            pltpu.VMEM((rows, HD), F32),
            pltpu.VMEM((2, own_rows * heads, HD), F32),
        ],
        compiler_params=pltpu.CompilerParams(vmem_limit_bytes=12 << 20),
        cost_estimate=pl.CostEstimate(flops=10**9, bytes_accessed=4 << 20, transcendentals=0),
    )(slot_of, lengths, *queries, new_kv, cache)


def project_kernel(count, rows, heads, *refs):
    taken = grouped(count)
    part_refs = refs[:taken]
    wo_ref, out_ref, joined, context = refs[taken:]
    parts = [piece(part_refs, count, s) for s in range(count)]

    def stats(part):
        tables = []
        for block in range(rows // LANES):
            at = rows + block * STATS
            table = part[at : at + STATS, :].astype(F32)
            tall = jnp.concatenate([table, jnp.zeros((LANES - STATS, LANES), F32)], axis=0)
            tables.append(tall.T)
        table = jnp.concatenate(tables, axis=0)
        return table[:, 0:1], table[:, 1:2] + table[:, 2:3]

    found = [stats(part) for part in parts]
    peak = functools.reduce(jnp.maximum, [m for m, _ in found])
    weights = [jnp.exp(m - peak) for m, _ in found]
    denominator = sum(w * l for w, (_, l) in zip(weights, found))
    numerator = sum(w * part[0:rows, :].astype(F32) for w, part in zip(weights, parts))
    joined[...] = numerator / denominator
    total = rows // heads
    for head in range(heads):
        context[:, head * HD : (head + 1) * HD] = joined[
            pl.ds(head, total, stride=heads), :
        ].astype(BF)
    out_ref[...] = jnp.dot(context[...], wo_ref[...], preferred_element_type=F32).astype(BF)


def project(parts, wo, count, total):
    heads = wo.shape[0] // HD
    rows = total * heads
    return pl.pallas_call(
        functools.partial(project_kernel, count, rows, heads),
        name="project",
        out_shape=jax.ShapeDtypeStruct((total, wo.shape[1]), BF),
        in_specs=[VMEM] * (len(parts) + 1),
        out_specs=VMEM,
        scratch_shapes=[
            pltpu.VMEM((rows, HD), F32),
            pltpu.VMEM((total, wo.shape[0]), BF),
        ],
        compiler_params=pltpu.CompilerParams(vmem_limit_bytes=(12 if len(parts) == count else 48) << 20),
        cost_estimate=pl.CostEstimate(flops=10**9, bytes_accessed=4 << 20, transcendentals=0),
    )(*parts, wo)


def residual_kernel(count, *refs):
    taken = grouped(count)
    part_refs = refs[:taken]
    resid_ref, gain_ref, attn_ref, out_ref, ordered = refs[taken:]
    me = lax.axis_index("tensor")
    for shift in range(count):
        ordered[source(part_refs, count, me, shift)] = piece(part_refs, count, shift)
    attention = sum(ordered[i].astype(F32) for i in range(count)).astype(BF)
    attn_ref[...] = attention
    hidden = resid_ref[...].astype(F32) + attention.astype(F32)
    squares = jnp.sum(hidden * hidden, axis=1, keepdims=True)
    width = hidden.shape[1]
    out_ref[:, 0:width] = (hidden * gain_ref[...].astype(F32)).astype(BF)
    high = squares.astype(BF).astype(F32)
    middle = (squares - high).astype(BF).astype(F32)
    low = squares - high - middle
    column = lax.broadcasted_iota(jnp.int32, (hidden.shape[0], LANES), 1)
    out_ref[:, width:] = jnp.where(
        column == 0, high, jnp.where(column == 1, middle, jnp.where(column == 2, low, 0.0))
    ).astype(BF)


def residual(parts, resid, gain, count):
    rows, width = resid.shape
    return pl.pallas_call(
        functools.partial(residual_kernel, count),
        name="residual",
        out_shape=(
            jax.ShapeDtypeStruct((rows, width), BF),
            jax.ShapeDtypeStruct((rows, width + LANES), BF),
        ),
        in_specs=[VMEM] * (len(parts) + 2),
        out_specs=(VMEM, VMEM),
        scratch_shapes=[pltpu.VMEM((count, rows, width), BF)],
        compiler_params=pltpu.CompilerParams(vmem_limit_bytes=8 << 20),
        cost_estimate=pl.CostEstimate(flops=10**8, bytes_accessed=1 << 20, transcendentals=0),
    )(*parts, resid, gain.reshape(1, width))


def experts_kernel(count, sharing, chunks, *refs):
    taken = grouped(count)
    part_refs = refs[:taken]
    ids_ref, logits_ref, gate_hbm, up_hbm, down_hbm = refs[taken : taken + 5]
    out_refs = refs[taken + 5 : 2 * taken + 5]
    spread, gate_buf, up_buf, down_buf, act, gate_sem, up_sem, down_sem = refs[2 * taken + 5 :]
    me = lax.axis_index("expert")
    depth, hidden_units = gate_buf.shape
    step = depth // chunks
    down_step = hidden_units // chunks
    copies = []
    for c in range(chunks):
        at = pl.ds(c * step, step)
        copies.append(
            (
                pltpu.make_async_copy(gate_hbm.at[at, :], gate_buf.at[at, :], gate_sem.at[c]),
                pltpu.make_async_copy(up_hbm.at[at, :], up_buf.at[at, :], up_sem.at[c]),
            )
        )
    down_copies = []
    for c in range(chunks):
        at = pl.ds(c * down_step, down_step)
        down_copies.append(
            pltpu.make_async_copy(down_hbm.at[at, :], down_buf.at[at, :], down_sem.at[c])
        )
    for pair in copies:
        pair[0].start()
        pair[1].start()
    for copy in down_copies:
        copy.start()
    rows = spread.shape[0]
    width = depth // count
    squares = jnp.zeros((rows, 1), F32)
    for shift in range(count):
        block = piece(part_refs, count, shift)
        at = source(part_refs, count, me, shift)
        spread[:, pl.ds(pl.multiple_of(at * width, width), width)] = block[:, 0:width]
        tail = block[:, width:].astype(F32)
        squares = squares + (tail[:, 0:1] + tail[:, 1:2] + tail[:, 2:3])
    inverse = lax.rsqrt(squares / depth + EPSILON)
    mine = me // sharing
    logits = logits_ref[...]
    first = 1.0 / (1.0 + jnp.exp(logits[1:2, :] - logits[0:1, :]))
    ids = ids_ref[...]
    mix_row = jnp.where(ids[0:1, :] == mine, first, 0.0) + jnp.where(
        ids[1:2, :] == mine, 1.0 - first, 0.0
    )
    eye = lax.broadcasted_iota(jnp.int32, (rows, rows), 0) == lax.broadcasted_iota(
        jnp.int32, (rows, rows), 1
    )
    mix = jnp.sum(jnp.where(eye, mix_row, 0.0), axis=1, keepdims=True)
    gate_sum = jnp.zeros((rows, hidden_units), F32)
    up_sum = jnp.zeros((rows, hidden_units), F32)
    for c in range(chunks):
        at = pl.ds(c * step, step)
        block = spread[:, at]
        copies[c][0].wait()
        gate_sum += jnp.dot(block, gate_buf[at, :], preferred_element_type=F32)
        copies[c][1].wait()
        up_sum += jnp.dot(block, up_buf[at, :], preferred_element_type=F32)
    gate_sum = gate_sum * inverse
    act[...] = (gate_sum / (1.0 + jnp.exp(-gate_sum)) * (up_sum * inverse)).astype(BF)
    for copy in down_copies:
        copy.wait()
    stacked = taken == 1
    for shift in range(count):
        at = target(stacked, count, me, shift)
        columns = pl.ds(pl.multiple_of(at * width, width), width)
        made = jnp.dot(act[...], down_buf[:, columns], preferred_element_type=F32)
        made = (made * mix).astype(BF)
        if stacked:
            out_refs[0][shift] = made
        else:
            out_refs[shift][...] = made


def experts(parts, ids, logits, gate, up, down, count):
    depth, hidden_units = gate.shape
    rows = ids.shape[0]
    width = depth // count
    stacked = len(parts) != count
    one = jax.ShapeDtypeStruct((rows, width), BF)
    out_shape = (
        (jax.ShapeDtypeStruct((count, rows, width), BF),) if stacked else tuple([one] * count)
    )
    chunks = 4
    hbm = lambda w: pltpu.with_memory_space_constraint(w, pltpu.HBM)
    return pl.pallas_call(
        functools.partial(experts_kernel, count, count // EXPERTS, chunks),
        name="experts",
        out_shape=out_shape,
        in_specs=[VMEM] * (len(parts) + 2) + [HBM] * 3,
        out_specs=tuple([VMEM] * len(out_shape)),
        scratch_shapes=[
            pltpu.VMEM((rows, depth), BF),
            pltpu.VMEM((depth, hidden_units), BF),
            pltpu.VMEM((depth, hidden_units), BF),
            pltpu.VMEM((hidden_units, depth), BF),
            pltpu.VMEM((rows, hidden_units), BF),
            pltpu.SemaphoreType.DMA((chunks,)),
            pltpu.SemaphoreType.DMA((chunks,)),
            pltpu.SemaphoreType.DMA((chunks,)),
        ],
        compiler_params=pltpu.CompilerParams(vmem_limit_bytes=58 << 20),
        cost_estimate=pl.CostEstimate(flops=10**10, bytes_accessed=50 << 20, transcendentals=0),
    )(*parts, ids.T, logits.T, hbm(gate), hbm(up), hbm(down))


def first_sum_kernel(count, other, *refs):
    taken = grouped(count)
    part_refs, out_refs = refs[:taken], refs[taken:]
    me = lax.axis_index("tensor")
    total = sum(piece(part_refs, count, s).astype(F32) for s in range(count))
    rows = total.shape[0] // other
    blocks = [total[i * rows : (i + 1) * rows, :] for i in range(other)]
    for shift in range(other):
        if grouped(other) == 1:
            out_refs[0][shift] = blocks[shift].astype(BF)
        else:
            at = target(False, other, me, shift)
            chosen = sum(jnp.where(at == i, blocks[i], 0.0) for i in range(other))
            out_refs[shift][...] = chosen.astype(BF)


def last_sum_kernel(count, *refs):
    taken = grouped(count)
    part_refs, out_ref = refs[:taken], refs[taken]
    out_ref[...] = sum(piece(part_refs, count, s).astype(F32) for s in range(count)).astype(BF)


def first_sum(parts, count, other, rows, width):
    one = (rows // other, width)
    if grouped(other) == 1:
        out_shape = (jax.ShapeDtypeStruct((other,) + one, BF),)
    else:
        out_shape = tuple([jax.ShapeDtypeStruct(one, BF)] * other)
    return pl.pallas_call(
        functools.partial(first_sum_kernel, count, other),
        name="first_sum",
        out_shape=out_shape,
        in_specs=[VMEM] * len(parts),
        out_specs=tuple([VMEM] * len(out_shape)),
        compiler_params=pltpu.CompilerParams(vmem_limit_bytes=8 << 20),
    )(*parts)


def last_sum(parts, count, shape):
    return pl.pallas_call(
        functools.partial(last_sum_kernel, count),
        name="last_sum",
        out_shape=jax.ShapeDtypeStruct(shape, BF),
        in_specs=[VMEM] * len(parts),
        out_specs=VMEM,
        compiler_params=pltpu.CompilerParams(vmem_limit_bytes=8 << 20),
    )(*parts)


def shards(
    kv_prefill,
    slot_of,
    lengths,
    query,
    new_kv,
    wo,
    resid,
    norm_gain,
    expert_ids,
    gate_logits,
    gate_weight_slabs,
    w_up,
    w_down,
):
    expert_count = lax.axis_size("expert")
    tensor_count = lax.axis_size("tensor")
    total, width = resid.shape
    slots, positions, _, kv_width = kv_prefill.shape
    queries = gather(query, "expert")
    cache = kv_prefill.reshape(slots, 2 * positions, kv_width)
    part = attend(slot_of, lengths, queries, new_kv, cache, expert_count)
    projected = project(gather(part, "expert"), wo, expert_count, total)
    attention, scaled = residual(gather(projected, "tensor"), resid, norm_gain, tensor_count)
    outgoing = experts(
        gather(scaled, "expert"),
        expert_ids,
        gate_logits,
        gate_weight_slabs[0],
        w_up[0],
        w_down[0],
        expert_count,
    )
    column_parts = first_sum(
        exchange(outgoing, "expert"), expert_count, tensor_count, total, width
    )
    moe_out = last_sum(
        exchange(column_parts, "tensor"), tensor_count, (total // tensor_count, width)
    )
    return (attention, moe_out)


def solution(mesh):
    return jax.shard_map(
        shards,
        mesh=mesh,
        in_specs=(
            P("groups", "expert", None, "tensor"),
            P("groups"),
            P("groups"),
            P(("groups", "expert"), "tensor"),
            P(("groups", "expert"), None, "tensor"),
            P("tensor", "expert"),
            P("groups", "expert"),
            P("expert"),
            P("groups", None),
            P("groups", None),
            P("expert", None, "tensor"),
            P("expert", None, "tensor"),
            P("expert", "tensor", None),
        ),
        out_specs=(P("groups", "expert"), P(("groups", "tensor"), "expert")),
        check_vma=False,
    )
```

```python
import functools
import math

import jax
import jax.numpy as jnp
from jax import lax
from jax.experimental import pallas as pl
from jax.experimental.pallas import tpu as pltpu
from jax.sharding import PartitionSpec as P

HEADS = 32
KVH = 8
HD = 128
EXPERTS = 4
EPSILON = 1e-05
MASKED = -1e30
LIVE = -1e29
LANES = 128
STATS = 16
MOST_PERMUTES = 4

BF = jnp.bfloat16
F32 = jnp.float32
VMEM = pl.BlockSpec(memory_space=pltpu.VMEM)
SMEM = pl.BlockSpec(memory_space=pltpu.SMEM)
HBM = pl.BlockSpec(memory_space=pltpu.HBM)


def gather(value, axis):
    count = lax.axis_size(axis)
    if count > MOST_PERMUTES:
        return [lax.all_gather(value, axis)]
    out = [value]
    for shift in range(1, count):
        out.append(lax.ppermute(value, axis, [(i, (i + shift) % count) for i in range(count)]))
    return out


def exchange(values, axis):
    count = lax.axis_size(axis)
    if count > MOST_PERMUTES:
        return [lax.all_to_all(values[0], axis, 0, 0, tiled=True)]
    out = [values[0]]
    for shift in range(1, count):
        out.append(
            lax.ppermute(values[shift], axis, [(i, (i + shift) % count) for i in range(count)])
        )
    return out


def piece(refs, count, shift):
    return refs[shift][...] if len(refs) == count else refs[0][shift]


def source(refs, count, me, shift):
    return lax.rem(me - shift + count, count) if len(refs) == count else shift


def target(stacked, count, me, shift):
    return shift if stacked else lax.rem(me + shift, count)


def grouped(count):
    return 1 if count > MOST_PERMUTES else count


def load_kernel(cuts, waits, *refs):
    count = len(cuts)
    sources, outs, sems = refs[:count], refs[count + waits : -1], refs[-1]
    copies = []
    for i, cut in enumerate(cuts):
        view = sources[i] if cut is None else sources[i].at[cut]
        copies.append(pltpu.make_async_copy(view, outs[i], sems.at[i]))
    for copy in copies:
        copy.start()
    for copy in copies:
        copy.wait()


def load(items, waits=()):
    hbm = lambda w: pltpu.with_memory_space_constraint(w, pltpu.HBM)
    size = sum(math.prod(shape) * array.dtype.itemsize for array, _, shape in items)
    return pl.pallas_call(
        functools.partial(load_kernel, [cut for _, cut, _ in items], len(waits)),
        name="load",
        out_shape=tuple(pltpu.VMEM(shape, array.dtype) for array, _, shape in items),
        in_specs=[HBM] * len(items) + [pl.BlockSpec(memory_space=pl.ANY)] * len(waits),
        out_specs=tuple([VMEM] * len(items)),
        scratch_shapes=[pltpu.SemaphoreType.DMA((len(items),))],
        compiler_params=pltpu.CompilerParams(vmem_limit_bytes=1 << 20),
        cost_estimate=pl.CostEstimate(flops=10**8, bytes_accessed=2 * size, transcendentals=0),
    )(*[hbm(array) for array, _, _ in items], *waits)


def whole(array):
    return (array, None, array.shape)


def rows_of(array, part, parts):
    step = array.shape[0] // parts
    return (array, (pl.ds(part * step, step), slice(None)), (step, array.shape[1]))


def attend_kernel(count, own_rows, kv_heads, group, positions, *refs):
    taken = grouped(count)
    slot_ref, length_ref = refs[0], refs[1]
    query_refs = refs[2 : 2 + taken]
    new_ref = refs[2 + taken]
    cache_refs = refs[3 + taken : 3 + taken + kv_heads]
    out_ref, q_rows, score, acc, fresh = refs[3 + taken + kv_heads :]
    me = lax.axis_index("expert")
    heads = kv_heads * group
    total = count * own_rows
    rows = total * heads
    width = 2 * positions
    scale = 1.0 / math.sqrt(HD)
    for shift in range(count):
        block = piece(query_refs, count, shift).astype(F32)
        where_to = source(query_refs, count, me, shift)
        for head in range(heads):
            q_rows[where_to, pl.ds(head, own_rows, stride=heads), :] = block[
                :, head * HD : (head + 1) * HD
            ]
    head_of_row = lax.broadcasted_iota(jnp.int32, (heads, HD), 0) // group
    lane = lax.broadcasted_iota(jnp.int32, (heads, width), 1)
    position = me * positions + lane // 2
    is_key = lax.rem(lane, 2) == 0

    def cached(b):
        at = slot_ref[b]
        return jnp.concatenate([ref[at] for ref in cache_refs], axis=1)

    def diagonal(parts):
        return sum(jnp.where(head_of_row == g, parts(g), 0.0) for g in range(kv_heads))

    def scores(b):
        owner, within = b // own_rows, lax.rem(b, own_rows)
        vectors = q_rows[owner, pl.ds(pl.multiple_of(within * heads, heads), heads), :]
        spread = jnp.concatenate(
            [jnp.where(head_of_row == g, vectors, 0.0) for g in range(kv_heads)], axis=1
        ).astype(BF)
        both = cached(b)
        found = (
            lax.dot_general(
                spread, both, (((1,), (1,)), ((), ())), preferred_element_type=F32
            )
            * scale
        )
        live = is_key & (position < length_ref[b])
        score[pl.ds(pl.multiple_of(b * heads, heads), heads), :] = jnp.where(live, found, MASKED)

    def values(b):
        at = pl.ds(pl.multiple_of(b * heads, heads), heads)
        both = cached(b)
        summed = jnp.dot(score[at, :].astype(BF), both, preferred_element_type=F32)
        acc[at, :] = diagonal(lambda g: summed[:, g * HD : (g + 1) * HD])

    def sweep(step):
        if total <= 16:
            for b in range(total):
                step(b)
        else:
            pl.loop(0, total)(step)

    sweep(scores)
    own = own_rows * heads
    new = new_ref[...].astype(F32)
    for b in range(own_rows):
        for g in range(kv_heads):
            at = b * heads + g * group
            for which in range(2):
                fresh[which, at : at + group, :] = jnp.broadcast_to(
                    new[b, which : which + 1, g * HD : (g + 1) * HD], (group, HD)
                )
    own_score = jnp.sum(q_rows[me] * fresh[0], axis=1, keepdims=True) * scale
    row = lax.broadcasted_iota(jnp.int32, (rows, 1), 0)
    at_home = (row >= me * own) & (row < (me + 1) * own)
    own_all = jnp.concatenate([own_score] * count, axis=0)
    own_all = jnp.where(at_home, own_all, MASKED)
    raw = score[...]
    peak = jnp.maximum(jnp.max(raw, axis=1, keepdims=True), own_all).astype(BF).astype(F32)
    weights = jnp.where(raw > LIVE, jnp.exp(raw - peak), 0.0)
    own_weight = jnp.where(at_home, jnp.exp(own_all - peak), 0.0)
    weight_sum = jnp.sum(weights, axis=1, keepdims=True) + own_weight
    score[...] = pltpu.roll(weights, 1, 1)
    sweep(values)
    fresh_all = jnp.concatenate([fresh[1]] * count, axis=0)
    out_ref[0:rows, :] = (acc[...] + own_weight * fresh_all).astype(BF)
    high = weight_sum.astype(BF).astype(F32)
    low = weight_sum - high
    column = lax.broadcasted_iota(jnp.int32, (rows, LANES), 1)
    table = jnp.where(
        column == 0, peak, jnp.where(column == 1, high, jnp.where(column == 2, low, 0.0))
    )
    for part in range(rows // LANES):
        turned = table[part * LANES : (part + 1) * LANES, :].T
        out_ref[rows + part * STATS : rows + (part + 1) * STATS, :] = turned[0:STATS, :].astype(BF)


def attend(slot_of, lengths, queries, new_kv, caches, count):
    own_rows, _, kv_width = new_kv.shape
    kv_heads = kv_width // HD
    group = HEADS // KVH
    heads = kv_heads * group
    positions = caches[0].shape[1] // 2
    rows = count * own_rows * heads
    return pl.pallas_call(
        functools.partial(attend_kernel, count, own_rows, kv_heads, group, positions),
        name="attend",
        out_shape=jax.ShapeDtypeStruct((rows + STATS * (rows // LANES), LANES), BF),
        in_specs=[SMEM, SMEM] + [VMEM] * (len(queries) + 1 + kv_heads),
        out_specs=VMEM,
        scratch_shapes=[
            pltpu.VMEM((count, own_rows * heads, HD), F32),
            pltpu.VMEM((rows, 2 * positions), F32),
            pltpu.VMEM((rows, HD), F32),
            pltpu.VMEM((2, own_rows * heads, HD), F32),
        ],
        compiler_params=pltpu.CompilerParams(vmem_limit_bytes=12 << 20),
        cost_estimate=pl.CostEstimate(flops=10**9, bytes_accessed=4 << 20, transcendentals=0),
    )(slot_of, lengths, *queries, new_kv, *caches)


def project_kernel(count, rows, heads, *refs):
    taken = grouped(count)
    part_refs = refs[:taken]
    wo_ref, out_ref, joined, context = refs[taken:]
    parts = [piece(part_refs, count, s) for s in range(count)]

    def stats(part):
        tables = []
        for block in range(rows // LANES):
            at = rows + block * STATS
            table = part[at : at + STATS, :].astype(F32)
            tall = jnp.concatenate([table, jnp.zeros((LANES - STATS, LANES), F32)], axis=0)
            tables.append(tall.T)
        table = jnp.concatenate(tables, axis=0)
        return table[:, 0:1], table[:, 1:2] + table[:, 2:3]

    found = [stats(part) for part in parts]
    peak = functools.reduce(jnp.maximum, [m for m, _ in found])
    weights = [jnp.exp(m - peak) for m, _ in found]
    denominator = sum(w * l for w, (_, l) in zip(weights, found))
    numerator = sum(w * part[0:rows, :].astype(F32) for w, part in zip(weights, parts))
    joined[...] = numerator / denominator
    total = rows // heads
    for head in range(heads):
        context[:, head * HD : (head + 1) * HD] = joined[
            pl.ds(head, total, stride=heads), :
        ].astype(BF)
    out_ref[...] = jnp.dot(context[...], wo_ref[...], preferred_element_type=F32).astype(BF)


def project(parts, wo, count, total):
    heads = wo.shape[0] // HD
    rows = total * heads
    return pl.pallas_call(
        functools.partial(project_kernel, count, rows, heads),
        name="project",
        out_shape=jax.ShapeDtypeStruct((total, wo.shape[1]), BF),
        in_specs=[VMEM] * (len(parts) + 1),
        out_specs=VMEM,
        scratch_shapes=[
            pltpu.VMEM((rows, HD), F32),
            pltpu.VMEM((total, wo.shape[0]), BF),
        ],
        compiler_params=pltpu.CompilerParams(vmem_limit_bytes=(12 if len(parts) == count else 48) << 20),
        cost_estimate=pl.CostEstimate(flops=10**9, bytes_accessed=4 << 20, transcendentals=0),
    )(*parts, wo)


def residual_kernel(count, *refs):
    taken = grouped(count)
    part_refs = refs[:taken]
    resid_ref, gain_ref, attn_ref, out_ref, ordered = refs[taken:]
    me = lax.axis_index("tensor")
    for shift in range(count):
        ordered[source(part_refs, count, me, shift)] = piece(part_refs, count, shift)
    attention = sum(ordered[i].astype(F32) for i in range(count)).astype(BF)
    attn_ref[...] = attention
    hidden = resid_ref[...].astype(F32) + attention.astype(F32)
    squares = jnp.sum(hidden * hidden, axis=1, keepdims=True)
    width = hidden.shape[1]
    gain = gain_ref[...].astype(F32).reshape(1, width)
    out_ref[:, 0:width] = (hidden * gain).astype(BF)
    high = squares.astype(BF).astype(F32)
    middle = (squares - high).astype(BF).astype(F32)
    low = squares - high - middle
    column = lax.broadcasted_iota(jnp.int32, (hidden.shape[0], LANES), 1)
    out_ref[:, width:] = jnp.where(
        column == 0, high, jnp.where(column == 1, middle, jnp.where(column == 2, low, 0.0))
    ).astype(BF)


def residual(parts, resid, gain, count):
    rows, width = resid.shape
    return pl.pallas_call(
        functools.partial(residual_kernel, count),
        name="residual",
        out_shape=(
            jax.ShapeDtypeStruct((rows, width), BF),
            jax.ShapeDtypeStruct((rows, width + LANES), BF),
        ),
        in_specs=[VMEM] * (len(parts) + 2),
        out_specs=(VMEM, VMEM),
        scratch_shapes=[pltpu.VMEM((count, rows, width), BF)],
        compiler_params=pltpu.CompilerParams(vmem_limit_bytes=8 << 20),
        cost_estimate=pl.CostEstimate(flops=10**8, bytes_accessed=1 << 20, transcendentals=0),
    )(*parts, resid, gain)


def experts_kernel(count, sharing, chunks, *refs):
    taken = grouped(count)
    part_refs, refs = refs[:taken], refs[taken:]
    ids_ref, logits_ref, refs = refs[0], refs[1], refs[2:]
    gate_refs, up_refs, refs = refs[:chunks], refs[chunks : 2 * chunks], refs[2 * chunks :]
    down_hbm, refs = refs[0], refs[1:]
    out_refs, refs = refs[:taken], refs[taken:]
    spread, down_buf, act, down_sem = refs
    me = lax.axis_index("expert")
    hidden_units, depth = down_buf.shape
    step = depth // chunks
    down_step = hidden_units // chunks
    down_copies = []
    for c in range(chunks):
        at = pl.ds(c * down_step, down_step)
        down_copies.append(
            pltpu.make_async_copy(down_hbm.at[at, :], down_buf.at[at, :], down_sem.at[c])
        )
    for copy in down_copies:
        copy.start()
    rows = spread.shape[0]
    width = depth // count
    squares = jnp.zeros((rows, 1), F32)
    for shift in range(count):
        block = piece(part_refs, count, shift)
        at = source(part_refs, count, me, shift)
        spread[:, pl.ds(pl.multiple_of(at * width, width), width)] = block[:, 0:width]
        tail = block[:, width:].astype(F32)
        squares = squares + (tail[:, 0:1] + tail[:, 1:2] + tail[:, 2:3])
    inverse = lax.rsqrt(squares / depth + EPSILON)
    mine = me // sharing
    logits = logits_ref[...]
    first = 1.0 / (1.0 + jnp.exp(logits[1:2, :] - logits[0:1, :]))
    ids = ids_ref[...]
    mix_row = jnp.where(ids[0:1, :] == mine, first, 0.0) + jnp.where(
        ids[1:2, :] == mine, 1.0 - first, 0.0
    )
    eye = lax.broadcasted_iota(jnp.int32, (rows, rows), 0) == lax.broadcasted_iota(
        jnp.int32, (rows, rows), 1
    )
    mix = jnp.sum(jnp.where(eye, mix_row, 0.0), axis=1, keepdims=True)
    gate_sum = jnp.zeros((rows, hidden_units), F32)
    up_sum = jnp.zeros((rows, hidden_units), F32)
    for c in range(chunks):
        block = spread[:, c * step : (c + 1) * step]
        gate_sum += jnp.dot(block, gate_refs[c][...], preferred_element_type=F32)
        up_sum += jnp.dot(block, up_refs[c][...], preferred_element_type=F32)
    gate_sum = gate_sum * inverse
    act[...] = (gate_sum / (1.0 + jnp.exp(-gate_sum)) * (up_sum * inverse)).astype(BF)
    for copy in down_copies:
        copy.wait()
    stacked = taken == 1
    for shift in range(count):
        at = target(stacked, count, me, shift)
        columns = pl.ds(pl.multiple_of(at * width, width), width)
        made = jnp.dot(act[...], down_buf[:, columns], preferred_element_type=F32)
        made = (made * mix).astype(BF)
        if stacked:
            out_refs[0][shift] = made
        else:
            out_refs[shift][...] = made


def experts(parts, ids, logits, gates, ups, down, count):
    hidden_units, depth = down.shape
    rows = ids.shape[1]
    width = depth // count
    chunks = len(gates)
    stacked = len(parts) != count
    one = pltpu.VMEM((rows, width), BF)
    out_shape = (pltpu.VMEM((count, rows, width), BF),) if stacked else tuple([one] * count)
    return pl.pallas_call(
        functools.partial(experts_kernel, count, count // EXPERTS, chunks),
        name="experts",
        out_shape=out_shape,
        in_specs=[VMEM] * (len(parts) + 2 + 2 * chunks) + [HBM],
        out_specs=tuple([VMEM] * len(out_shape)),
        scratch_shapes=[
            pltpu.VMEM((rows, depth), BF),
            pltpu.VMEM((hidden_units, depth), BF),
            pltpu.VMEM((rows, hidden_units), BF),
            pltpu.SemaphoreType.DMA((chunks,)),
        ],
        compiler_params=pltpu.CompilerParams(vmem_limit_bytes=19 << 20),
        cost_estimate=pl.CostEstimate(flops=10**10, bytes_accessed=50 << 20, transcendentals=0),
    )(
        *[
            pltpu.with_memory_space_constraint(w, pltpu.VMEM)
            for w in (*parts, ids, logits, *gates, *ups)
        ],
        pltpu.with_memory_space_constraint(down, pltpu.HBM),
    )


def first_sum_kernel(count, other, *refs):
    taken = grouped(count)
    part_refs, out_refs = refs[:taken], refs[taken:]
    me = lax.axis_index("tensor")
    total = sum(piece(part_refs, count, s).astype(F32) for s in range(count))
    rows = total.shape[0] // other
    blocks = [total[i * rows : (i + 1) * rows, :] for i in range(other)]
    for shift in range(other):
        if grouped(other) == 1:
            out_refs[0][shift] = blocks[shift].astype(BF)
        else:
            at = target(False, other, me, shift)
            chosen = sum(jnp.where(at == i, blocks[i], 0.0) for i in range(other))
            out_refs[shift][...] = chosen.astype(BF)


def last_sum_kernel(count, *refs):
    taken = grouped(count)
    part_refs, out_ref = refs[:taken], refs[taken]
    out_ref[...] = sum(piece(part_refs, count, s).astype(F32) for s in range(count)).astype(BF)


def first_sum(parts, count, other, rows, width):
    one = (rows // other, width)
    if grouped(other) == 1:
        out_shape = (jax.ShapeDtypeStruct((other,) + one, BF),)
    else:
        out_shape = tuple([jax.ShapeDtypeStruct(one, BF)] * other)
    return pl.pallas_call(
        functools.partial(first_sum_kernel, count, other),
        name="first_sum",
        out_shape=out_shape,
        in_specs=[VMEM] * len(parts),
        out_specs=tuple([VMEM] * len(out_shape)),
        compiler_params=pltpu.CompilerParams(vmem_limit_bytes=8 << 20),
    )(*parts)


def last_sum(parts, count, shape):
    return pl.pallas_call(
        functools.partial(last_sum_kernel, count),
        name="last_sum",
        out_shape=jax.ShapeDtypeStruct(shape, BF),
        in_specs=[VMEM] * len(parts),
        out_specs=VMEM,
        compiler_params=pltpu.CompilerParams(vmem_limit_bytes=8 << 20),
    )(*parts)


def shards(
    kv_prefill,
    slot_of,
    lengths,
    query,
    new_kv,
    wo,
    resid,
    norm_gain,
    expert_ids,
    gate_logits,
    gate_weight_slabs,
    w_up,
    w_down,
):
    expert_count = lax.axis_size("expert")
    tensor_count = lax.axis_size("tensor")
    total, width = resid.shape
    slots, positions, _, kv_width = kv_prefill.shape
    gate, up, down = gate_weight_slabs[0], w_up[0], w_down[0]
    chunks = 4
    part_of = lambda w, c: rows_of(w, c, chunks)
    kv_heads = kv_width // HD
    queries = gather(query, "expert")
    head_shape = (slots, positions, 2, HD)
    heads = [
        (kv_prefill, (slice(None), slice(None), slice(None), pl.ds(g * HD, HD)), head_shape)
        for g in range(kv_heads)
    ]
    loaded = load([whole(query), whole(new_kv), *heads, part_of(gate, 0)])
    if len(queries) == expert_count:
        queries[0] = loaded[0]
    fresh, caches, gate_0 = loaded[1], loaded[2:-1], loaded[-1]
    caches = [cache.reshape(slots, 2 * positions, HD) for cache in caches]
    part = attend(slot_of, lengths, queries, fresh, caches, expert_count)
    parts = gather(part, "expert")
    wo_here, resid_here, gain_here, ids, logits, gate_1, up_0, up_1 = load(
        [
            whole(wo),
            whole(resid),
            whole(norm_gain),
            whole(expert_ids.T),
            whole(gate_logits.T),
            part_of(gate, 1),
            part_of(up, 0),
            part_of(up, 1),
        ],
        [part],
    )
    projected = project(parts, wo_here, expert_count, total)
    attention, scaled = residual(gather(projected, "tensor"), resid_here, gain_here, tensor_count)
    blocks = gather(scaled, "expert")
    gate_2, up_2, gate_3, up_3 = load(
        [part_of(gate, 2), part_of(up, 2), part_of(gate, 3), part_of(up, 3)], [scaled]
    )
    outgoing = experts(
        blocks,
        ids,
        logits,
        [gate_0, gate_1, gate_2, gate_3],
        [up_0, up_1, up_2, up_3],
        down,
        expert_count,
    )
    column_parts = first_sum(
        exchange(outgoing, "expert"), expert_count, tensor_count, total, width
    )
    moe_out = last_sum(
        exchange(column_parts, "tensor"), tensor_count, (total // tensor_count, width)
    )
    return (attention, moe_out)


def solution(mesh):
    return jax.shard_map(
        shards,
        mesh=mesh,
        in_specs=(
            P("groups", "expert", None, "tensor"),
            P("groups"),
            P("groups"),
            P(("groups", "expert"), "tensor"),
            P(("groups", "expert"), None, "tensor"),
            P("tensor", "expert"),
            P("groups", "expert"),
            P("expert"),
            P("groups", None),
            P("groups", None),
            P("expert", None, "tensor"),
            P("expert", None, "tensor"),
            P("expert", "tensor", None),
        ),
        out_specs=(P("groups", "expert"), P(("groups", "tensor"), "expert")),
        check_vma=False,
    )
```

```python
import functools
import math

import jax
import jax.numpy as jnp
from jax import lax
from jax.experimental import pallas as pl
from jax.experimental.pallas import tpu as pltpu
from jax.sharding import PartitionSpec as P

HEADS = 32
KVH = 8
HD = 128
EXPERTS = 4
EPSILON = 1e-05
MASKED = -1e30
LIVE = -1e29
LANES = 128
STATS = 16
MOST_PERMUTES = 4
GATE_PARTS = 4

BF = jnp.bfloat16
F32 = jnp.float32
VMEM = pl.BlockSpec(memory_space=pltpu.VMEM)
SMEM = pl.BlockSpec(memory_space=pltpu.SMEM)
HBM = pl.BlockSpec(memory_space=pltpu.HBM)


def gather(value, axis):
    count = lax.axis_size(axis)
    if count > MOST_PERMUTES:
        return [lax.all_gather(value, axis)]
    out = [value]
    for shift in range(1, count):
        out.append(lax.ppermute(value, axis, [(i, (i + shift) % count) for i in range(count)]))
    return out


def exchange(values, axis):
    count = lax.axis_size(axis)
    if count > MOST_PERMUTES:
        return [lax.all_to_all(values[0], axis, 0, 0, tiled=True)]
    out = [values[0]]
    for shift in range(1, count):
        out.append(
            lax.ppermute(values[shift], axis, [(i, (i + shift) % count) for i in range(count)])
        )
    return out


def piece(refs, count, shift):
    return refs[shift][...] if len(refs) == count else refs[0][shift]


def source(refs, count, me, shift):
    return lax.rem(me - shift + count, count) if len(refs) == count else shift


def target(stacked, count, me, shift):
    return shift if stacked else lax.rem(me + shift, count)


def grouped(count):
    return 1 if count > MOST_PERMUTES else count


def load_kernel(cuts, waits, *refs):
    count = len(cuts)
    sources, outs, sems = refs[:count], refs[count + waits : -1], refs[-1]
    copies = []
    for i, cut in enumerate(cuts):
        view = sources[i] if cut is None else sources[i].at[cut]
        copies.append(pltpu.make_async_copy(view, outs[i], sems.at[i]))
    for copy in copies:
        copy.start()
    for copy in copies:
        copy.wait()


def load(items, waits=(), flops=10**8):
    hbm = lambda w: pltpu.with_memory_space_constraint(w, pltpu.HBM)
    return pl.pallas_call(
        functools.partial(load_kernel, [cut for _, cut, _ in items], len(waits)),
        name="load",
        out_shape=tuple(pltpu.VMEM(shape, array.dtype) for array, _, shape in items),
        in_specs=[HBM] * len(items) + [pl.BlockSpec(memory_space=pl.ANY)] * len(waits),
        out_specs=tuple([VMEM] * len(items)),
        scratch_shapes=[pltpu.SemaphoreType.DMA((len(items),))],
        compiler_params=pltpu.CompilerParams(vmem_limit_bytes=1 << 20),
        cost_estimate=pl.CostEstimate(flops=flops, bytes_accessed=1000, transcendentals=0),
    )(*[hbm(array) for array, _, _ in items], *waits)


def whole(array):
    return (array, None, array.shape)


def rows_of(array, part, parts):
    step = array.shape[0] // parts
    return (array, (pl.ds(part * step, step), slice(None)), (step, array.shape[1]))


def attend_kernel(count, own_rows, kv_heads, group, positions, *refs):
    taken = grouped(count)
    slot_ref, length_ref = refs[0], refs[1]
    query_refs = refs[2 : 2 + taken]
    new_ref = refs[2 + taken]
    cache_refs = refs[3 + taken : 3 + taken + kv_heads]
    out_ref, q_rows, score, acc, fresh = refs[3 + taken + kv_heads :]
    me = lax.axis_index("expert")
    heads = kv_heads * group
    total = count * own_rows
    rows = total * heads
    width = 2 * positions
    scale = 1.0 / math.sqrt(HD)
    for shift in range(count):
        block = piece(query_refs, count, shift).astype(F32)
        where_to = source(query_refs, count, me, shift)
        for head in range(heads):
            q_rows[where_to, pl.ds(head, own_rows, stride=heads), :] = block[
                :, head * HD : (head + 1) * HD
            ]
    head_of_row = lax.broadcasted_iota(jnp.int32, (heads, HD), 0) // group
    lane = lax.broadcasted_iota(jnp.int32, (heads, width), 1)
    position = me * positions + lane // 2
    is_key = lax.rem(lane, 2) == 0

    def cached(b):
        at = slot_ref[b]
        return jnp.concatenate([ref[at] for ref in cache_refs], axis=1)

    def diagonal(parts):
        return sum(jnp.where(head_of_row == g, parts(g), 0.0) for g in range(kv_heads))

    def scores(b):
        owner, within = b // own_rows, lax.rem(b, own_rows)
        vectors = q_rows[owner, pl.ds(pl.multiple_of(within * heads, heads), heads), :]
        spread = jnp.concatenate(
            [jnp.where(head_of_row == g, vectors, 0.0) for g in range(kv_heads)], axis=1
        ).astype(BF)
        both = cached(b)
        found = (
            lax.dot_general(
                spread, both, (((1,), (1,)), ((), ())), preferred_element_type=F32
            )
            * scale
        )
        live = is_key & (position < length_ref[b])
        score[pl.ds(pl.multiple_of(b * heads, heads), heads), :] = jnp.where(live, found, MASKED)

    def values(b):
        at = pl.ds(pl.multiple_of(b * heads, heads), heads)
        both = cached(b)
        summed = jnp.dot(score[at, :].astype(BF), both, preferred_element_type=F32)
        acc[at, :] = diagonal(lambda g: summed[:, g * HD : (g + 1) * HD])

    def sweep(step):
        if total <= 16:
            for b in range(total):
                step(b)
        else:
            pl.loop(0, total)(step)

    sweep(scores)
    own = own_rows * heads
    new = new_ref[...].astype(F32)
    for b in range(own_rows):
        for g in range(kv_heads):
            at = b * heads + g * group
            for which in range(2):
                fresh[which, at : at + group, :] = jnp.broadcast_to(
                    new[b, which : which + 1, g * HD : (g + 1) * HD], (group, HD)
                )
    own_score = jnp.sum(q_rows[me] * fresh[0], axis=1, keepdims=True) * scale
    row = lax.broadcasted_iota(jnp.int32, (rows, 1), 0)
    at_home = (row >= me * own) & (row < (me + 1) * own)
    own_all = jnp.concatenate([own_score] * count, axis=0)
    own_all = jnp.where(at_home, own_all, MASKED)
    raw = score[...]
    peak = jnp.maximum(jnp.max(raw, axis=1, keepdims=True), own_all).astype(BF).astype(F32)
    weights = jnp.where(raw > LIVE, jnp.exp(raw - peak), 0.0)
    own_weight = jnp.where(at_home, jnp.exp(own_all - peak), 0.0)
    weight_sum = jnp.sum(weights, axis=1, keepdims=True) + own_weight
    score[...] = pltpu.roll(weights, 1, 1)
    sweep(values)
    fresh_all = jnp.concatenate([fresh[1]] * count, axis=0)
    out_ref[0:rows, :] = (acc[...] + own_weight * fresh_all).astype(BF)
    high = weight_sum.astype(BF).astype(F32)
    low = weight_sum - high
    column = lax.broadcasted_iota(jnp.int32, (rows, LANES), 1)
    table = jnp.where(
        column == 0, peak, jnp.where(column == 1, high, jnp.where(column == 2, low, 0.0))
    )
    for part in range(rows // LANES):
        turned = table[part * LANES : (part + 1) * LANES, :].T
        out_ref[rows + part * STATS : rows + (part + 1) * STATS, :] = turned[0:STATS, :].astype(BF)


def attend(slot_of, lengths, queries, new_kv, caches, count):
    own_rows, _, kv_width = new_kv.shape
    kv_heads = kv_width // HD
    group = HEADS // KVH
    heads = kv_heads * group
    positions = caches[0].shape[1] // 2
    rows = count * own_rows * heads
    return pl.pallas_call(
        functools.partial(attend_kernel, count, own_rows, kv_heads, group, positions),
        name="attend",
        out_shape=jax.ShapeDtypeStruct((rows + STATS * (rows // LANES), LANES), BF),
        in_specs=[SMEM, SMEM] + [VMEM] * (len(queries) + 1 + kv_heads),
        out_specs=VMEM,
        scratch_shapes=[
            pltpu.VMEM((count, own_rows * heads, HD), F32),
            pltpu.VMEM((rows, 2 * positions), F32),
            pltpu.VMEM((rows, HD), F32),
            pltpu.VMEM((2, own_rows * heads, HD), F32),
        ],
        compiler_params=pltpu.CompilerParams(vmem_limit_bytes=6 << 20),
        cost_estimate=pl.CostEstimate(flops=10**8, bytes_accessed=1000, transcendentals=0),
    )(slot_of, lengths, *queries, new_kv, *caches)


def project_kernel(count, rows, heads, *refs):
    taken = grouped(count)
    part_refs = refs[:taken]
    wo_ref, out_ref, joined, context = refs[taken:]
    parts = [piece(part_refs, count, s) for s in range(count)]

    def stats(part):
        tables = []
        for block in range(rows // LANES):
            at = rows + block * STATS
            table = part[at : at + STATS, :].astype(F32)
            tall = jnp.concatenate([table, jnp.zeros((LANES - STATS, LANES), F32)], axis=0)
            tables.append(tall.T)
        table = jnp.concatenate(tables, axis=0)
        return table[:, 0:1], table[:, 1:2] + table[:, 2:3]

    found = [stats(part) for part in parts]
    peak = functools.reduce(jnp.maximum, [m for m, _ in found])
    weights = [jnp.exp(m - peak) for m, _ in found]
    denominator = sum(w * l for w, (_, l) in zip(weights, found))
    numerator = sum(w * part[0:rows, :].astype(F32) for w, part in zip(weights, parts))
    joined[...] = numerator / denominator
    total = rows // heads
    for head in range(heads):
        context[:, head * HD : (head + 1) * HD] = joined[
            pl.ds(head, total, stride=heads), :
        ].astype(BF)
    out_ref[...] = jnp.dot(context[...], wo_ref[...], preferred_element_type=F32).astype(BF)


def project(parts, wo, count, total):
    heads = wo.shape[0] // HD
    rows = total * heads
    return pl.pallas_call(
        functools.partial(project_kernel, count, rows, heads),
        name="project",
        out_shape=jax.ShapeDtypeStruct((total, wo.shape[1]), BF),
        in_specs=[VMEM] * (len(parts) + 1),
        out_specs=VMEM,
        scratch_shapes=[
            pltpu.VMEM((rows, HD), F32),
            pltpu.VMEM((total, wo.shape[0]), BF),
        ],
        compiler_params=pltpu.CompilerParams(vmem_limit_bytes=(4 if len(parts) == count else 48) << 20),
        cost_estimate=pl.CostEstimate(flops=10**11, bytes_accessed=1000, transcendentals=0),
    )(*parts, wo)


def residual_kernel(count, *refs):
    taken = grouped(count)
    part_refs = refs[:taken]
    resid_ref, gain_ref, attn_ref, out_ref, ordered = refs[taken:]
    me = lax.axis_index("tensor")
    for shift in range(count):
        ordered[source(part_refs, count, me, shift)] = piece(part_refs, count, shift)
    attention = sum(ordered[i].astype(F32) for i in range(count)).astype(BF)
    attn_ref[...] = attention
    hidden = resid_ref[...].astype(F32) + attention.astype(F32)
    squares = jnp.sum(hidden * hidden, axis=1, keepdims=True)
    width = hidden.shape[1]
    gain = gain_ref[...].astype(F32).reshape(1, width)
    out_ref[:, 0:width] = (hidden * gain).astype(BF)
    high = squares.astype(BF).astype(F32)
    middle = (squares - high).astype(BF).astype(F32)
    low = squares - high - middle
    column = lax.broadcasted_iota(jnp.int32, (hidden.shape[0], LANES), 1)
    out_ref[:, width:] = jnp.where(
        column == 0, high, jnp.where(column == 1, middle, jnp.where(column == 2, low, 0.0))
    ).astype(BF)


def residual(parts, resid, gain, count):
    rows, width = resid.shape
    return pl.pallas_call(
        functools.partial(residual_kernel, count),
        name="residual",
        out_shape=(
            jax.ShapeDtypeStruct((rows, width), BF),
            jax.ShapeDtypeStruct((rows, width + LANES), BF),
        ),
        in_specs=[VMEM] * (len(parts) + 2),
        out_specs=(VMEM, VMEM),
        scratch_shapes=[pltpu.VMEM((count, rows, width), BF)],
        compiler_params=pltpu.CompilerParams(vmem_limit_bytes=4 << 20),
        cost_estimate=pl.CostEstimate(flops=10**8, bytes_accessed=1000, transcendentals=0),
    )(*parts, resid, gain)


def experts_kernel(count, sharing, gates, *refs):
    taken = grouped(count)
    part_refs, refs = refs[:taken], refs[taken:]
    ids_ref, logits_ref, refs = refs[0], refs[1], refs[2:]
    up_ref, down_ref, refs = *refs[:2], refs[2:]
    gate_refs, refs = refs[:gates], refs[gates:]
    out_refs, refs = refs[:taken], refs[taken:]
    spread, act = refs
    me = lax.axis_index("expert")
    depth = up_ref.shape[0]
    rows = spread.shape[0]
    width = depth // count
    squares = jnp.zeros((rows, 1), F32)
    for shift in range(count):
        block = piece(part_refs, count, shift)
        at = source(part_refs, count, me, shift)
        spread[:, pl.ds(pl.multiple_of(at * width, width), width)] = block[:, 0:width]
        tail = block[:, width:].astype(F32)
        squares = squares + (tail[:, 0:1] + tail[:, 1:2] + tail[:, 2:3])
    inverse = lax.rsqrt(squares / depth + EPSILON)
    mine = me // sharing
    logits = logits_ref[...]
    first = 1.0 / (1.0 + jnp.exp(logits[1:2, :] - logits[0:1, :]))
    ids = ids_ref[...]
    mix_row = jnp.where(ids[0:1, :] == mine, first, 0.0) + jnp.where(
        ids[1:2, :] == mine, 1.0 - first, 0.0
    )
    eye = lax.broadcasted_iota(jnp.int32, (rows, rows), 0) == lax.broadcasted_iota(
        jnp.int32, (rows, rows), 1
    )
    mix = jnp.sum(jnp.where(eye, mix_row, 0.0), axis=1, keepdims=True)
    step = depth // gates
    gate_sum = sum(
        jnp.dot(spread[:, i * step : (i + 1) * step], ref[...], preferred_element_type=F32)
        for i, ref in enumerate(gate_refs)
    )
    up_sum = jnp.dot(spread[...], up_ref[...], preferred_element_type=F32)
    gate_sum = gate_sum * inverse
    act[...] = (gate_sum / (1.0 + jnp.exp(-gate_sum)) * (up_sum * inverse)).astype(BF)
    stacked = taken == 1
    for shift in range(count):
        at = target(stacked, count, me, shift)
        columns = pl.ds(pl.multiple_of(at * width, width), width)
        made = jnp.dot(act[...], down_ref[:, columns], preferred_element_type=F32)
        made = (made * mix).astype(BF)
        if stacked:
            out_refs[0][shift] = made
        else:
            out_refs[shift][...] = made


def experts(parts, ids, logits, gates, up, down, count):
    hidden_units, depth = down.shape
    rows = ids.shape[1]
    width = depth // count
    stacked = len(parts) != count
    one = pltpu.VMEM((rows, width), BF)
    out_shape = (pltpu.VMEM((count, rows, width), BF),) if stacked else tuple([one] * count)
    return pl.pallas_call(
        functools.partial(experts_kernel, count, count // EXPERTS, len(gates)),
        name="experts",
        out_shape=out_shape,
        in_specs=[VMEM] * (len(parts) + 4 + len(gates)),
        out_specs=tuple([VMEM] * len(out_shape)),
        scratch_shapes=[
            pltpu.VMEM((rows, depth), BF),
            pltpu.VMEM((rows, hidden_units), BF),
        ],
        compiler_params=pltpu.CompilerParams(vmem_limit_bytes=(16 if stacked else 4) << 20),
        cost_estimate=pl.CostEstimate(flops=10**8, bytes_accessed=1000, transcendentals=0),
    )(*parts, ids, logits, up, down, *gates)


def first_sum_kernel(count, other, *refs):
    taken = grouped(count)
    part_refs, out_refs = refs[:taken], refs[taken:]
    me = lax.axis_index("tensor")
    total = sum(piece(part_refs, count, s).astype(F32) for s in range(count))
    rows = total.shape[0] // other
    blocks = [total[i * rows : (i + 1) * rows, :] for i in range(other)]
    for shift in range(other):
        if grouped(other) == 1:
            out_refs[0][shift] = blocks[shift].astype(BF)
        else:
            at = target(False, other, me, shift)
            chosen = sum(jnp.where(at == i, blocks[i], 0.0) for i in range(other))
            out_refs[shift][...] = chosen.astype(BF)


def last_sum_kernel(count, *refs):
    taken = grouped(count)
    part_refs, out_ref = refs[:taken], refs[taken]
    out_ref[...] = sum(piece(part_refs, count, s).astype(F32) for s in range(count)).astype(BF)


def first_sum(parts, count, other, rows, width):
    one = (rows // other, width)
    if grouped(other) == 1:
        out_shape = (jax.ShapeDtypeStruct((other,) + one, BF),)
    else:
        out_shape = tuple([jax.ShapeDtypeStruct(one, BF)] * other)
    return pl.pallas_call(
        functools.partial(first_sum_kernel, count, other),
        name="first_sum",
        out_shape=out_shape,
        in_specs=[VMEM] * len(parts),
        out_specs=tuple([VMEM] * len(out_shape)),
        compiler_params=pltpu.CompilerParams(vmem_limit_bytes=4 << 20),
    )(*parts)


def last_sum(parts, count, shape):
    return pl.pallas_call(
        functools.partial(last_sum_kernel, count),
        name="last_sum",
        out_shape=jax.ShapeDtypeStruct(shape, BF),
        in_specs=[VMEM] * len(parts),
        out_specs=VMEM,
        compiler_params=pltpu.CompilerParams(vmem_limit_bytes=4 << 20),
    )(*parts)


def shards(
    kv_prefill,
    slot_of,
    lengths,
    query,
    new_kv,
    wo,
    resid,
    norm_gain,
    expert_ids,
    gate_logits,
    gate_weight_slabs,
    w_up,
    w_down,
):
    expert_count = lax.axis_size("expert")
    tensor_count = lax.axis_size("tensor")
    total, width = resid.shape
    slots, positions, _, kv_width = kv_prefill.shape
    kv_heads = kv_width // HD
    queries = gather(query, "expert")
    head_shape = (slots, positions, 2, HD)
    heads = [
        (kv_prefill, (slice(None), slice(None), slice(None), pl.ds(g * HD, HD)), head_shape)
        for g in range(kv_heads)
    ]
    gate = gate_weight_slabs[0]
    loaded = load([whole(query), whole(new_kv), *heads, rows_of(gate, 0, GATE_PARTS), rows_of(gate, 1, GATE_PARTS)])
    if len(queries) == expert_count:
        queries[0] = loaded[0]
    fresh, caches = loaded[1], loaded[2 : 2 + kv_heads]
    gate_0 = loaded[2 + kv_heads]
    gate_1 = loaded[3 + kv_heads]
    caches = [cache.reshape(slots, 2 * positions, HD) for cache in caches]
    part = attend(slot_of, lengths, queries, fresh, caches, expert_count)
    parts = gather(part, "expert")
    wo_here, resid_here, gain_here, gate_2, gate_3 = load([whole(wo), whole(resid), whole(norm_gain), rows_of(gate, 2, GATE_PARTS), rows_of(gate, 3, GATE_PARTS)], [part])
    projected = project(parts, wo_here, expert_count, total)
    partials = gather(projected, "tensor")
    attention, scaled = residual(partials, resid_here, gain_here, tensor_count)
    blocks = gather(scaled, "expert")
    outgoing = experts(
        blocks,
        expert_ids.T,
        gate_logits.T,
        (gate_0, gate_1, gate_2, gate_3),
        w_up[0],
        w_down[0],
        expert_count,
    )
    column_parts = first_sum(
        exchange(outgoing, "expert"), expert_count, tensor_count, total, width
    )
    moe_out = last_sum(
        exchange(column_parts, "tensor"), tensor_count, (total // tensor_count, width)
    )
    return (attention, moe_out)


def solution(mesh):
    return jax.shard_map(
        shards,
        mesh=mesh,
        in_specs=(
            P("groups", "expert", None, "tensor"),
            P("groups"),
            P("groups"),
            P(("groups", "expert"), "tensor"),
            P(("groups", "expert"), None, "tensor"),
            P("tensor", "expert"),
            P("groups", "expert"),
            P("expert"),
            P("groups", None),
            P("groups", None),
            P("expert", None, "tensor"),
            P("expert", None, "tensor"),
            P("expert", "tensor", None),
        ),
        out_specs=(P("groups", "expert"), P(("groups", "tensor"), "expert")),
        check_vma=False,
    )
```

```python
import functools
import math

import jax
import jax.numpy as jnp
from jax import lax
from jax.experimental import pallas as pl
from jax.experimental.pallas import tpu as pltpu
from jax.sharding import PartitionSpec as P

HEADS = 32
KVH = 8
HD = 128
EXPERTS = 4
EPSILON = 1e-05
MASKED = -1e30
LIVE = -1e29
LANES = 128
STATS = 16
MOST_PERMUTES = 4
GATE_PARTS = 4
EARLY = (0, 3, 2, 1)

BF = jnp.bfloat16
F32 = jnp.float32
VMEM = pl.BlockSpec(memory_space=pltpu.VMEM)
SMEM = pl.BlockSpec(memory_space=pltpu.SMEM)
HBM = pl.BlockSpec(memory_space=pltpu.HBM)


def gather(value, axis):
    count = lax.axis_size(axis)
    if count > MOST_PERMUTES:
        return [lax.all_gather(value, axis)]
    out = [value]
    for shift in range(1, count):
        out.append(lax.ppermute(value, axis, [(i, (i + shift) % count) for i in range(count)]))
    return out


def exchange(values, axis):
    count = lax.axis_size(axis)
    if count > MOST_PERMUTES:
        return [lax.all_to_all(values[0], axis, 0, 0, tiled=True)]
    out = [values[0]]
    for shift in range(1, count):
        out.append(
            lax.ppermute(values[shift], axis, [(i, (i + shift) % count) for i in range(count)])
        )
    return out


def piece(refs, count, shift):
    return refs[shift][...] if len(refs) == count else refs[0][shift]


def source(refs, count, me, shift):
    return lax.rem(me - shift + count, count) if len(refs) == count else shift


def target(stacked, count, me, shift):
    return shift if stacked else lax.rem(me + shift, count)


def grouped(count):
    return 1 if count > MOST_PERMUTES else count


def load_kernel(cuts, waits, *refs):
    count = len(cuts)
    sources, outs, sems = refs[:count], refs[count + waits : -1], refs[-1]
    copies = []
    for i, cut in enumerate(cuts):
        view = sources[i] if cut is None else sources[i].at[cut() if callable(cut) else cut]
        copies.append(pltpu.make_async_copy(view, outs[i], sems.at[i]))
    for copy in copies:
        copy.start()
    for copy in copies:
        copy.wait()


def load(items, waits=(), flops=10**8):
    hbm = lambda w: pltpu.with_memory_space_constraint(w, pltpu.HBM)
    return pl.pallas_call(
        functools.partial(load_kernel, [cut for _, cut, _ in items], len(waits)),
        name="load",
        out_shape=tuple(pltpu.VMEM(shape, array.dtype) for array, _, shape in items),
        in_specs=[HBM] * len(items) + [pl.BlockSpec(memory_space=pl.ANY)] * len(waits),
        out_specs=tuple([VMEM] * len(items)),
        scratch_shapes=[pltpu.SemaphoreType.DMA((len(items),))],
        compiler_params=pltpu.CompilerParams(vmem_limit_bytes=1 << 20),
        cost_estimate=pl.CostEstimate(flops=flops, bytes_accessed=1000, transcendentals=0),
    )(*[hbm(array) for array, _, _ in items], *waits)


def whole(array):
    return (array, None, array.shape)


def rows_at(part, count, step, relative):
    if relative:
        part = lax.rem(lax.axis_index("expert") - part + count, count)
        return (pl.ds(pl.multiple_of(part * step, step), step), slice(None))
    return (pl.ds(part * step, step), slice(None))


def rows_of(array, part, count, relative):
    step = array.shape[0] // count
    cut = functools.partial(rows_at, part, count, step, relative)
    return (array, cut, (step, array.shape[1]))


def attend_kernel(count, own_rows, kv_heads, group, positions, cut, *refs):
    taken = grouped(count)
    slot_ref, length_ref = refs[0], refs[1]
    query_refs = refs[2 : 2 + taken]
    new_ref = refs[2 + taken]
    cache_refs = refs[3 + taken : 3 + taken + kv_heads]
    chunk_hbm, out_ref, chunk_ref, q_rows, score, acc, fresh, chunk_sem = refs[
        3 + taken + kv_heads :
    ]
    chunk_copy = pltpu.make_async_copy(chunk_hbm.at[cut()], chunk_ref, chunk_sem)
    chunk_copy.start()
    me = lax.axis_index("expert")
    heads = kv_heads * group
    total = count * own_rows
    rows = total * heads
    width = 2 * positions
    scale = 1.0 / math.sqrt(HD)
    for shift in range(count):
        block = piece(query_refs, count, shift).astype(F32)
        where_to = source(query_refs, count, me, shift)
        for head in range(heads):
            q_rows[where_to, pl.ds(head, own_rows, stride=heads), :] = block[
                :, head * HD : (head + 1) * HD
            ]
    head_of_row = lax.broadcasted_iota(jnp.int32, (heads, HD), 0) // group
    lane = lax.broadcasted_iota(jnp.int32, (heads, width), 1)
    position = me * positions + lane // 2
    is_key = lax.rem(lane, 2) == 0

    def cached(b):
        at = slot_ref[b]
        return jnp.concatenate([ref[at] for ref in cache_refs], axis=1)

    def diagonal(parts):
        return sum(jnp.where(head_of_row == g, parts(g), 0.0) for g in range(kv_heads))

    def scores(b):
        owner, within = b // own_rows, lax.rem(b, own_rows)
        vectors = q_rows[owner, pl.ds(pl.multiple_of(within * heads, heads), heads), :]
        spread = jnp.concatenate(
            [jnp.where(head_of_row == g, vectors, 0.0) for g in range(kv_heads)], axis=1
        ).astype(BF)
        both = cached(b)
        found = (
            lax.dot_general(
                spread, both, (((1,), (1,)), ((), ())), preferred_element_type=F32
            )
            * scale
        )
        live = is_key & (position < length_ref[b])
        score[pl.ds(pl.multiple_of(b * heads, heads), heads), :] = jnp.where(live, found, MASKED)

    def values(b):
        at = pl.ds(pl.multiple_of(b * heads, heads), heads)
        both = cached(b)
        summed = jnp.dot(score[at, :].astype(BF), both, preferred_element_type=F32)
        acc[at, :] = diagonal(lambda g: summed[:, g * HD : (g + 1) * HD])

    def sweep(step):
        if total <= 16:
            for b in range(total):
                step(b)
        else:
            pl.loop(0, total)(step)

    sweep(scores)
    own = own_rows * heads
    new = new_ref[...].astype(F32)
    for b in range(own_rows):
        for g in range(kv_heads):
            at = b * heads + g * group
            for which in range(2):
                fresh[which, at : at + group, :] = jnp.broadcast_to(
                    new[b, which : which + 1, g * HD : (g + 1) * HD], (group, HD)
                )
    own_score = jnp.sum(q_rows[me] * fresh[0], axis=1, keepdims=True) * scale
    row = lax.broadcasted_iota(jnp.int32, (rows, 1), 0)
    at_home = (row >= me * own) & (row < (me + 1) * own)
    own_all = jnp.concatenate([own_score] * count, axis=0)
    own_all = jnp.where(at_home, own_all, MASKED)
    raw = score[...]
    peak = jnp.maximum(jnp.max(raw, axis=1, keepdims=True), own_all).astype(BF).astype(F32)
    weights = jnp.where(raw > LIVE, jnp.exp(raw - peak), 0.0)
    own_weight = jnp.where(at_home, jnp.exp(own_all - peak), 0.0)
    weight_sum = jnp.sum(weights, axis=1, keepdims=True) + own_weight
    score[...] = pltpu.roll(weights, 1, 1)
    sweep(values)
    fresh_all = jnp.concatenate([fresh[1]] * count, axis=0)
    out_ref[0:rows, :] = (acc[...] + own_weight * fresh_all).astype(BF)
    high = weight_sum.astype(BF).astype(F32)
    low = weight_sum - high
    column = lax.broadcasted_iota(jnp.int32, (rows, LANES), 1)
    table = jnp.where(
        column == 0, peak, jnp.where(column == 1, high, jnp.where(column == 2, low, 0.0))
    )
    for part in range(rows // LANES):
        turned = table[part * LANES : (part + 1) * LANES, :].T
        out_ref[rows + part * STATS : rows + (part + 1) * STATS, :] = turned[0:STATS, :].astype(BF)
    chunk_copy.wait()


def attend(slot_of, lengths, queries, new_kv, caches, chunk, count):
    own_rows, _, kv_width = new_kv.shape
    kv_heads = kv_width // HD
    group = HEADS // KVH
    heads = kv_heads * group
    positions = caches[0].shape[1] // 2
    rows = count * own_rows * heads
    source_array, cut, shape = chunk
    return pl.pallas_call(
        functools.partial(attend_kernel, count, own_rows, kv_heads, group, positions, cut),
        name="attend",
        out_shape=(
            pltpu.VMEM((rows + STATS * (rows // LANES), LANES), BF),
            pltpu.VMEM(shape, BF),
        ),
        in_specs=[SMEM, SMEM] + [VMEM] * (len(queries) + 1 + kv_heads) + [HBM],
        out_specs=(VMEM, VMEM),
        scratch_shapes=[
            pltpu.VMEM((count, own_rows * heads, HD), F32),
            pltpu.VMEM((rows, 2 * positions), F32),
            pltpu.VMEM((rows, HD), F32),
            pltpu.VMEM((2, own_rows * heads, HD), F32),
            pltpu.SemaphoreType.DMA,
        ],
        compiler_params=pltpu.CompilerParams(vmem_limit_bytes=6 << 20),
        cost_estimate=pl.CostEstimate(flops=10**8, bytes_accessed=1000, transcendentals=0),
    )(
        slot_of,
        lengths,
        *queries,
        new_kv,
        *caches,
        pltpu.with_memory_space_constraint(source_array, pltpu.HBM),
    )


def project_kernel(count, rows, heads, *refs):
    taken = grouped(count)
    part_refs = refs[:taken]
    wo_ref, out_ref, joined, context = refs[taken:]
    parts = [piece(part_refs, count, s) for s in range(count)]

    def stats(part):
        tables = []
        for block in range(rows // LANES):
            at = rows + block * STATS
            table = part[at : at + STATS, :].astype(F32)
            tall = jnp.concatenate([table, jnp.zeros((LANES - STATS, LANES), F32)], axis=0)
            tables.append(tall.T)
        table = jnp.concatenate(tables, axis=0)
        return table[:, 0:1], table[:, 1:2] + table[:, 2:3]

    found = [stats(part) for part in parts]
    peak = functools.reduce(jnp.maximum, [m for m, _ in found])
    weights = [jnp.exp(m - peak) for m, _ in found]
    denominator = sum(w * l for w, (_, l) in zip(weights, found))
    numerator = sum(w * part[0:rows, :].astype(F32) for w, part in zip(weights, parts))
    joined[...] = numerator / denominator
    total = rows // heads
    for head in range(heads):
        context[:, head * HD : (head + 1) * HD] = joined[
            pl.ds(head, total, stride=heads), :
        ].astype(BF)
    out_ref[...] = jnp.dot(context[...], wo_ref[...], preferred_element_type=F32).astype(BF)


def project(parts, wo, count, total):
    heads = wo.shape[0] // HD
    rows = total * heads
    return pl.pallas_call(
        functools.partial(project_kernel, count, rows, heads),
        name="project",
        out_shape=jax.ShapeDtypeStruct((total, wo.shape[1]), BF),
        in_specs=[VMEM] * (len(parts) + 1),
        out_specs=VMEM,
        scratch_shapes=[
            pltpu.VMEM((rows, HD), F32),
            pltpu.VMEM((total, wo.shape[0]), BF),
        ],
        compiler_params=pltpu.CompilerParams(vmem_limit_bytes=(4 if len(parts) == count else 48) << 20),
        cost_estimate=pl.CostEstimate(flops=10**11, bytes_accessed=1000, transcendentals=0),
    )(*parts, wo)


def residual_kernel(count, *refs):
    taken = grouped(count)
    part_refs = refs[:taken]
    resid_ref, gain_ref, attn_ref, out_ref, ordered = refs[taken:]
    me = lax.axis_index("tensor")
    for shift in range(count):
        ordered[source(part_refs, count, me, shift)] = piece(part_refs, count, shift)
    attention = sum(ordered[i].astype(F32) for i in range(count)).astype(BF)
    attn_ref[...] = attention
    hidden = resid_ref[...].astype(F32) + attention.astype(F32)
    squares = jnp.sum(hidden * hidden, axis=1, keepdims=True)
    width = hidden.shape[1]
    gain = gain_ref[...].astype(F32).reshape(1, width)
    out_ref[:, 0:width] = (hidden * gain).astype(BF)
    high = squares.astype(BF).astype(F32)
    middle = (squares - high).astype(BF).astype(F32)
    low = squares - high - middle
    column = lax.broadcasted_iota(jnp.int32, (hidden.shape[0], LANES), 1)
    out_ref[:, width:] = jnp.where(
        column == 0, high, jnp.where(column == 1, middle, jnp.where(column == 2, low, 0.0))
    ).astype(BF)


def residual(parts, resid, gain, count):
    rows, width = resid.shape
    return pl.pallas_call(
        functools.partial(residual_kernel, count),
        name="residual",
        out_shape=(
            pltpu.VMEM((rows, width), BF),
            pltpu.VMEM((rows, width + LANES), BF),
        ),
        in_specs=[VMEM] * (len(parts) + 2),
        out_specs=(VMEM, VMEM),
        scratch_shapes=[pltpu.VMEM((count, rows, width), BF)],
        compiler_params=pltpu.CompilerParams(vmem_limit_bytes=4 << 20),
        cost_estimate=pl.CostEstimate(flops=10**8, bytes_accessed=1000, transcendentals=0),
    )(*parts, resid, gain)


def gate_kernel(*refs):
    block_ref, gate_ref, out_ref = refs[0], refs[1], refs[-1]
    block = block_ref[:, 0 : gate_ref.shape[0]]
    made = jnp.dot(block, gate_ref[...], preferred_element_type=F32)
    out_ref[...] = made if len(refs) == 3 else made + refs[2][...]


def gate_product(block, gate, before=()):
    return pl.pallas_call(
        gate_kernel,
        name="gate_product",
        out_shape=pltpu.VMEM((block.shape[0], gate.shape[1]), F32),
        in_specs=[VMEM] * (2 + len(before)),
        out_specs=VMEM,
        compiler_params=pltpu.CompilerParams(vmem_limit_bytes=2 << 20),
        cost_estimate=pl.CostEstimate(flops=10**8, bytes_accessed=1000, transcendentals=0),
    )(block, gate, *before)


def experts_kernel(count, sharing, gates, cut, *refs):
    taken = grouped(count)
    stacked = taken == 1
    part_refs, refs = refs[:taken], refs[taken:]
    ids_ref, logits_ref, up_ref, down_ref, last_hbm, refs = *refs[:5], refs[5:]
    before_refs, refs = refs[:gates], refs[gates:]
    out_refs, refs = refs[:taken], refs[taken:]
    spread, act, last_gate, last_sem = refs
    last_copy = pltpu.make_async_copy(last_hbm.at[cut()], last_gate, last_sem)
    last_copy.start()
    me = lax.axis_index("expert")
    depth = up_ref.shape[0]
    rows = spread.shape[0]
    width = depth // count
    squares = jnp.zeros((rows, 1), F32)
    for shift in range(count):
        block = piece(part_refs, count, shift)
        at = source(part_refs, count, me, shift)
        spread[:, pl.ds(pl.multiple_of(at * width, width), width)] = block[:, 0:width]
        tail = block[:, width:].astype(F32)
        squares = squares + (tail[:, 0:1] + tail[:, 1:2] + tail[:, 2:3])
    inverse = lax.rsqrt(squares / depth + EPSILON)
    mine = me // sharing
    logits = logits_ref[...]
    first = 1.0 / (1.0 + jnp.exp(logits[1:2, :] - logits[0:1, :]))
    ids = ids_ref[...]
    mix_row = jnp.where(ids[0:1, :] == mine, first, 0.0) + jnp.where(
        ids[1:2, :] == mine, 1.0 - first, 0.0
    )
    eye = lax.broadcasted_iota(jnp.int32, (rows, rows), 0) == lax.broadcasted_iota(
        jnp.int32, (rows, rows), 1
    )
    mix = jnp.sum(jnp.where(eye, mix_row, 0.0), axis=1, keepdims=True)
    up_sum = jnp.dot(spread[...], up_ref[...], preferred_element_type=F32)
    last_copy.wait()
    step = last_gate.shape[0]
    if stacked:
        gate_sum = jnp.dot(
            spread[:, depth - step :], last_gate[...], preferred_element_type=F32
        )
        for i, ref in enumerate(before_refs):
            gate_sum += jnp.dot(
                spread[:, i * step : (i + 1) * step], ref[...], preferred_element_type=F32
            )
    else:
        gate_sum = before_refs[0][...] + jnp.dot(
            part_refs[1][:, 0:width], last_gate[...], preferred_element_type=F32
        )
    gate_sum = gate_sum * inverse
    act[...] = (gate_sum / (1.0 + jnp.exp(-gate_sum)) * (up_sum * inverse)).astype(BF)
    for shift in range(count):
        at = target(stacked, count, me, shift)
        columns = pl.ds(pl.multiple_of(at * width, width), width)
        made = jnp.dot(act[...], down_ref[:, columns], preferred_element_type=F32)
        made = (made * mix).astype(BF)
        if stacked:
            out_refs[0][shift] = made
        else:
            out_refs[shift][...] = made


def experts(parts, ids, logits, up, down, last, before, count):
    hidden_units, depth = down.shape
    rows = ids.shape[1]
    width = depth // count
    stacked = len(parts) != count
    one = pltpu.VMEM((rows, width), BF)
    out_shape = (pltpu.VMEM((count, rows, width), BF),) if stacked else tuple([one] * count)
    gate, cut, shape = last
    return pl.pallas_call(
        functools.partial(experts_kernel, count, count // EXPERTS, len(before), cut),
        name="experts",
        out_shape=out_shape,
        in_specs=[VMEM] * (len(parts) + 4) + [HBM] + [VMEM] * len(before),
        out_specs=tuple([VMEM] * len(out_shape)),
        scratch_shapes=[
            pltpu.VMEM((rows, depth), BF),
            pltpu.VMEM((rows, hidden_units), BF),
            pltpu.VMEM(shape, BF),
            pltpu.SemaphoreType.DMA,
        ],
        compiler_params=pltpu.CompilerParams(vmem_limit_bytes=(20 if stacked else 7) << 20),
        cost_estimate=pl.CostEstimate(flops=10**8, bytes_accessed=1000, transcendentals=0),
    )(
        *parts,
        ids,
        logits,
        up,
        down,
        pltpu.with_memory_space_constraint(gate, pltpu.HBM),
        *before,
    )


def first_sum_kernel(count, other, *refs):
    taken = grouped(count)
    part_refs, out_refs = refs[:taken], refs[taken:]
    me = lax.axis_index("tensor")
    total = sum(piece(part_refs, count, s).astype(F32) for s in range(count))
    rows = total.shape[0] // other
    blocks = [total[i * rows : (i + 1) * rows, :] for i in range(other)]
    for shift in range(other):
        if grouped(other) == 1:
            out_refs[0][shift] = blocks[shift].astype(BF)
        else:
            at = target(False, other, me, shift)
            chosen = sum(jnp.where(at == i, blocks[i], 0.0) for i in range(other))
            out_refs[shift][...] = chosen.astype(BF)


def last_sum_kernel(count, *refs):
    taken = grouped(count)
    part_refs, out_ref = refs[:taken], refs[taken]
    out_ref[...] = sum(piece(part_refs, count, s).astype(F32) for s in range(count)).astype(BF)


def first_sum(parts, count, other, rows, width):
    one = (rows // other, width)
    if grouped(other) == 1:
        out_shape = (jax.ShapeDtypeStruct((other,) + one, BF),)
    else:
        out_shape = tuple([jax.ShapeDtypeStruct(one, BF)] * other)
    return pl.pallas_call(
        functools.partial(first_sum_kernel, count, other),
        name="first_sum",
        out_shape=out_shape,
        in_specs=[VMEM] * len(parts),
        out_specs=tuple([VMEM] * len(out_shape)),
        compiler_params=pltpu.CompilerParams(vmem_limit_bytes=4 << 20),
    )(*parts)


def last_sum(parts, count, shape):
    return pl.pallas_call(
        functools.partial(last_sum_kernel, count),
        name="last_sum",
        out_shape=jax.ShapeDtypeStruct(shape, BF),
        in_specs=[VMEM] * len(parts),
        out_specs=VMEM,
        compiler_params=pltpu.CompilerParams(vmem_limit_bytes=4 << 20),
    )(*parts)


def shards(
    kv_prefill,
    slot_of,
    lengths,
    query,
    new_kv,
    wo,
    resid,
    norm_gain,
    expert_ids,
    gate_logits,
    gate_weight_slabs,
    w_up,
    w_down,
):
    expert_count = lax.axis_size("expert")
    tensor_count = lax.axis_size("tensor")
    total, width = resid.shape
    slots, positions, _, kv_width = kv_prefill.shape
    kv_heads = kv_width // HD
    queries = gather(query, "expert")
    relative = len(queries) == expert_count
    chunk_count = expert_count if relative else GATE_PARTS
    gate = gate_weight_slabs[0]
    rows = lambda i: rows_of(gate, i, chunk_count, relative)
    order = EARLY if relative else tuple(range(chunk_count))
    head_shape = (slots, positions, 2, HD)
    heads = [
        (kv_prefill, (slice(None), slice(None), slice(None), pl.ds(g * HD, HD)), head_shape)
        for g in range(kv_heads)
    ]
    loaded = load([whole(query), whole(new_kv), *heads, rows(order[0])])
    if relative:
        queries[0] = loaded[0]
    fresh, caches, gate_0 = loaded[1], loaded[2 : 2 + kv_heads], loaded[2 + kv_heads]
    caches = [cache.reshape(slots, 2 * positions, HD) for cache in caches]
    part, gate_1 = attend(
        slot_of, lengths, queries, fresh, caches, rows(order[1]), expert_count
    )
    parts = gather(part, "expert")
    wo_here, resid_here, gain_here, gate_2 = load(
        [whole(wo), whole(resid), whole(norm_gain), rows(order[2])], [part]
    )
    projected = project(parts, wo_here, expert_count, total)
    partials = gather(projected, "tensor")
    attention, scaled = residual(partials, resid_here, gain_here, tensor_count)
    blocks = gather(scaled, "expert")
    before = [gate_0, gate_1, gate_2]
    if relative:
        made = []
        for shift, chunk in zip(order, before):
            made = [gate_product(blocks[shift], chunk, made)]
        before = made
    outgoing = experts(
        blocks,
        expert_ids.T,
        gate_logits.T,
        w_up[0],
        w_down[0],
        rows(order[3]),
        before,
        expert_count,
    )
    column_parts = first_sum(
        exchange(outgoing, "expert"), expert_count, tensor_count, total, width
    )
    moe_out = last_sum(
        exchange(column_parts, "tensor"), tensor_count, (total // tensor_count, width)
    )
    return (attention, moe_out)


def solution(mesh):
    return jax.shard_map(
        shards,
        mesh=mesh,
        in_specs=(
            P("groups", "expert", None, "tensor"),
            P("groups"),
            P("groups"),
            P(("groups", "expert"), "tensor"),
            P(("groups", "expert"), None, "tensor"),
            P("tensor", "expert"),
            P("groups", "expert"),
            P("expert"),
            P("groups", None),
            P("groups", None),
            P("expert", None, "tensor"),
            P("expert", None, "tensor"),
            P("expert", "tensor", None),
        ),
        out_specs=(P("groups", "expert"), P(("groups", "tensor"), "expert")),
        check_vma=False,
    )
```

```python
import functools
import math

import jax
import jax.numpy as jnp
from jax import lax
from jax.experimental import pallas as pl
from jax.experimental.pallas import tpu as pltpu
from jax.sharding import PartitionSpec as P

HEADS = 32
KVH = 8
HD = 128
EXPERTS = 4
EPSILON = 1e-05
MASKED = -1e30
LIVE = -1e29
LANES = 128
STATS = 16
MOST_PERMUTES = 4
CHUNKS = 4
TILE = 512

BF = jnp.bfloat16
F32 = jnp.float32
VMEM = pl.BlockSpec(memory_space=pltpu.VMEM)
SMEM = pl.BlockSpec(memory_space=pltpu.SMEM)
HBM = pl.BlockSpec(memory_space=pltpu.HBM)


def gather(value, axis):
    count = lax.axis_size(axis)
    if count > MOST_PERMUTES:
        return [lax.all_gather(value, axis)]
    out = [value]
    for shift in range(1, count):
        out.append(lax.ppermute(value, axis, [(i, (i + shift) % count) for i in range(count)]))
    return out


def exchange(values, axis):
    count = lax.axis_size(axis)
    if count > MOST_PERMUTES:
        return [lax.all_to_all(values[0], axis, 0, 0, tiled=True)]
    out = [values[0]]
    for shift in range(1, count):
        out.append(
            lax.ppermute(values[shift], axis, [(i, (i + shift) % count) for i in range(count)])
        )
    return out


def piece(refs, count, shift):
    return refs[shift][...] if len(refs) == count else refs[0][shift]


def source(refs, count, me, shift):
    return lax.rem(me - shift + count, count) if len(refs) == count else shift


def target(stacked, count, me, shift):
    return shift if stacked else lax.rem(me + shift, count)


def grouped(count):
    return 1 if count > MOST_PERMUTES else count


def load_kernel(cuts, waits, *refs):
    count = len(cuts)
    sources, outs, sems = refs[:count], refs[count + waits : -1], refs[-1]
    copies = []
    for i, cut in enumerate(cuts):
        view = sources[i] if cut is None else sources[i].at[cut() if callable(cut) else cut]
        copies.append(pltpu.make_async_copy(view, outs[i], sems.at[i]))
    for copy in copies:
        copy.start()
    for copy in copies:
        copy.wait()


def load(items, waits=(), flops=10**8):
    hbm = lambda w: pltpu.with_memory_space_constraint(w, pltpu.HBM)
    return pl.pallas_call(
        functools.partial(load_kernel, [cut for _, cut, _ in items], len(waits)),
        name="load",
        out_shape=tuple(pltpu.VMEM(shape, array.dtype) for array, _, shape in items),
        in_specs=[HBM] * len(items) + [pl.BlockSpec(memory_space=pl.ANY)] * len(waits),
        out_specs=tuple([VMEM] * len(items)),
        scratch_shapes=[pltpu.SemaphoreType.DMA((len(items),))],
        compiler_params=pltpu.CompilerParams(vmem_limit_bytes=1 << 20),
        cost_estimate=pl.CostEstimate(flops=flops, bytes_accessed=1000, transcendentals=0),
    )(*[hbm(array) for array, _, _ in items], *waits)


def whole(array):
    return (array, None, array.shape)


def rows_at(part, count, step, relative):
    if relative:
        part = lax.rem(lax.axis_index("expert") - part + count, count)
        return (pl.ds(pl.multiple_of(part * step, step), step), slice(None))
    return (pl.ds(part * step, step), slice(None))


def rows_of(array, part, count, relative):
    step = array.shape[0] // count
    cut = functools.partial(rows_at, part, count, step, relative)
    return (array, cut, (step, array.shape[1]))


def with_copy(copies, work):
    for copy in copies:
        copy.start()
    pl.when(lax.axis_index("expert") >= 0)(work)
    for copy in copies:
        copy.wait()


def attend_kernel(count, own_rows, kv_heads, group, positions, cut, *refs):
    taken = grouped(count)
    slot_ref, length_ref = refs[0], refs[1]
    query_refs = refs[2 : 2 + taken]
    new_ref = refs[2 + taken]
    cache_refs = refs[3 + taken : 3 + taken + kv_heads]
    refs = refs[3 + taken + kv_heads :]
    attend_body = functools.partial(
        attend_block,
        (count, own_rows, kv_heads, group, positions),
        (slot_ref, length_ref, query_refs, new_ref, cache_refs),
    )
    if cut is None:
        attend_body(*refs)
        return
    chunk_hbm, out_ref, chunk_ref, *scratch, chunk_sem = refs
    with_copy(
        [pltpu.make_async_copy(chunk_hbm.at[cut()], chunk_ref, chunk_sem)],
        lambda: attend_body(out_ref, *scratch),
    )


def attend_block(sizes, inputs, out_ref, q_rows, score, acc, fresh):
    count, own_rows, kv_heads, group, positions = sizes
    slot_ref, length_ref, query_refs, new_ref, cache_refs = inputs
    me = lax.axis_index("expert")
    heads = kv_heads * group
    total = count * own_rows
    rows = total * heads
    width = 2 * positions
    scale = 1.0 / math.sqrt(HD)
    for shift in range(count):
        block = piece(query_refs, count, shift).astype(F32)
        where_to = source(query_refs, count, me, shift)
        for head in range(heads):
            q_rows[where_to, pl.ds(head, own_rows, stride=heads), :] = block[
                :, head * HD : (head + 1) * HD
            ]
    head_of_row = lax.broadcasted_iota(jnp.int32, (heads, HD), 0) // group
    lane = lax.broadcasted_iota(jnp.int32, (heads, width), 1)
    position = me * positions + lane // 2
    is_key = lax.rem(lane, 2) == 0

    def cached(b):
        at = slot_ref[b]
        return jnp.concatenate([ref[at] for ref in cache_refs], axis=1)

    def diagonal(parts):
        return sum(jnp.where(head_of_row == g, parts(g), 0.0) for g in range(kv_heads))

    def scores(b):
        owner, within = b // own_rows, lax.rem(b, own_rows)
        vectors = q_rows[owner, pl.ds(pl.multiple_of(within * heads, heads), heads), :]
        spread = jnp.concatenate(
            [jnp.where(head_of_row == g, vectors, 0.0) for g in range(kv_heads)], axis=1
        ).astype(BF)
        both = cached(b)
        found = (
            lax.dot_general(
                spread, both, (((1,), (1,)), ((), ())), preferred_element_type=F32
            )
            * scale
        )
        live = is_key & (position < length_ref[b])
        score[pl.ds(pl.multiple_of(b * heads, heads), heads), :] = jnp.where(live, found, MASKED)

    def values(b):
        at = pl.ds(pl.multiple_of(b * heads, heads), heads)
        both = cached(b)
        summed = jnp.dot(score[at, :].astype(BF), both, preferred_element_type=F32)
        acc[at, :] = diagonal(lambda g: summed[:, g * HD : (g + 1) * HD])

    def sweep(step):
        if total <= 16:
            for b in range(total):
                step(b)
        else:
            pl.loop(0, total)(step)

    sweep(scores)
    own = own_rows * heads
    new = new_ref[...].astype(F32)
    for b in range(own_rows):
        for g in range(kv_heads):
            at = b * heads + g * group
            for which in range(2):
                fresh[which, at : at + group, :] = jnp.broadcast_to(
                    new[b, which : which + 1, g * HD : (g + 1) * HD], (group, HD)
                )
    own_score = jnp.sum(q_rows[me] * fresh[0], axis=1, keepdims=True) * scale
    row = lax.broadcasted_iota(jnp.int32, (rows, 1), 0)
    at_home = (row >= me * own) & (row < (me + 1) * own)
    own_all = jnp.concatenate([own_score] * count, axis=0)
    own_all = jnp.where(at_home, own_all, MASKED)
    raw = score[...]
    peak = jnp.maximum(jnp.max(raw, axis=1, keepdims=True), own_all).astype(BF).astype(F32)
    weights = jnp.where(raw > LIVE, jnp.exp(raw - peak), 0.0)
    own_weight = jnp.where(at_home, jnp.exp(own_all - peak), 0.0)
    weight_sum = jnp.sum(weights, axis=1, keepdims=True) + own_weight
    score[...] = pltpu.roll(weights, 1, 1)
    sweep(values)
    fresh_all = jnp.concatenate([fresh[1]] * count, axis=0)
    out_ref[0:rows, :] = (acc[...] + own_weight * fresh_all).astype(BF)
    high = weight_sum.astype(BF).astype(F32)
    low = weight_sum - high
    column = lax.broadcasted_iota(jnp.int32, (rows, LANES), 1)
    table = jnp.where(
        column == 0, peak, jnp.where(column == 1, high, jnp.where(column == 2, low, 0.0))
    )
    for part in range(rows // LANES):
        turned = table[part * LANES : (part + 1) * LANES, :].T
        out_ref[rows + part * STATS : rows + (part + 1) * STATS, :] = turned[0:STATS, :].astype(BF)


def attend(slot_of, lengths, queries, new_kv, caches, chunk, count):
    own_rows, _, kv_width = new_kv.shape
    kv_heads = kv_width // HD
    group = HEADS // KVH
    heads = kv_heads * group
    positions = caches[0].shape[1] // 2
    rows = count * own_rows * heads
    out_shape = [pltpu.VMEM((rows + STATS * (rows // LANES), LANES), BF)]
    scratch_shapes = [
        pltpu.VMEM((count, own_rows * heads, HD), F32),
        pltpu.VMEM((rows, 2 * positions), F32),
        pltpu.VMEM((rows, HD), F32),
        pltpu.VMEM((2, own_rows * heads, HD), F32),
    ]
    cut, more = None, []
    if chunk is not None:
        array, cut, shape = chunk
        more = [pltpu.with_memory_space_constraint(array, pltpu.HBM)]
        out_shape.append(pltpu.VMEM(shape, BF))
        scratch_shapes.append(pltpu.SemaphoreType.DMA)
    return pl.pallas_call(
        functools.partial(attend_kernel, count, own_rows, kv_heads, group, positions, cut),
        name="attend",
        out_shape=tuple(out_shape),
        in_specs=[SMEM, SMEM] + [VMEM] * (len(queries) + 1 + kv_heads) + [HBM] * len(more),
        out_specs=tuple([VMEM] * len(out_shape)),
        scratch_shapes=scratch_shapes,
        compiler_params=pltpu.CompilerParams(vmem_limit_bytes=6 << 20),
        cost_estimate=pl.CostEstimate(flops=10**8, bytes_accessed=1000, transcendentals=0),
    )(slot_of, lengths, *queries, new_kv, *caches, *more)


def project_kernel(count, rows, heads, *refs):
    taken = grouped(count)
    part_refs = refs[:taken]
    wo_ref, out_ref, joined, context = refs[taken:]
    parts = [piece(part_refs, count, s) for s in range(count)]

    def stats(part):
        tables = []
        for block in range(rows // LANES):
            at = rows + block * STATS
            table = part[at : at + STATS, :].astype(F32)
            tall = jnp.concatenate([table, jnp.zeros((LANES - STATS, LANES), F32)], axis=0)
            tables.append(tall.T)
        table = jnp.concatenate(tables, axis=0)
        return table[:, 0:1], table[:, 1:2] + table[:, 2:3]

    found = [stats(part) for part in parts]
    peak = functools.reduce(jnp.maximum, [m for m, _ in found])
    weights = [jnp.exp(m - peak) for m, _ in found]
    denominator = sum(w * l for w, (_, l) in zip(weights, found))
    numerator = sum(w * part[0:rows, :].astype(F32) for w, part in zip(weights, parts))
    joined[...] = numerator / denominator
    total = rows // heads
    for head in range(heads):
        context[:, head * HD : (head + 1) * HD] = joined[
            pl.ds(head, total, stride=heads), :
        ].astype(BF)
    out_ref[...] = jnp.dot(context[...], wo_ref[...], preferred_element_type=F32).astype(BF)


def project(parts, wo, count, total):
    heads = wo.shape[0] // HD
    rows = total * heads
    return pl.pallas_call(
        functools.partial(project_kernel, count, rows, heads),
        name="project",
        out_shape=jax.ShapeDtypeStruct((total, wo.shape[1]), BF),
        in_specs=[VMEM] * (len(parts) + 1),
        out_specs=VMEM,
        scratch_shapes=[
            pltpu.VMEM((rows, HD), F32),
            pltpu.VMEM((total, wo.shape[0]), BF),
        ],
        compiler_params=pltpu.CompilerParams(vmem_limit_bytes=(4 if len(parts) == count else 48) << 20),
        cost_estimate=pl.CostEstimate(flops=10**11, bytes_accessed=1000, transcendentals=0),
    )(*parts, wo)


def residual_kernel(count, *refs):
    taken = grouped(count)
    part_refs = refs[:taken]
    resid_ref, gain_ref, attn_ref, out_ref, ordered = refs[taken:]
    me = lax.axis_index("tensor")
    for shift in range(count):
        ordered[source(part_refs, count, me, shift)] = piece(part_refs, count, shift)
    attention = sum(ordered[i].astype(F32) for i in range(count)).astype(BF)
    attn_ref[...] = attention
    hidden = resid_ref[...].astype(F32) + attention.astype(F32)
    squares = jnp.sum(hidden * hidden, axis=1, keepdims=True)
    width = hidden.shape[1]
    gain = gain_ref[...].astype(F32).reshape(1, width)
    out_ref[:, 0:width] = (hidden * gain).astype(BF)
    high = squares.astype(BF).astype(F32)
    middle = (squares - high).astype(BF).astype(F32)
    low = squares - high - middle
    column = lax.broadcasted_iota(jnp.int32, (hidden.shape[0], LANES), 1)
    out_ref[:, width:] = jnp.where(
        column == 0, high, jnp.where(column == 1, middle, jnp.where(column == 2, low, 0.0))
    ).astype(BF)


def residual(parts, resid, gain, count):
    rows, width = resid.shape
    return pl.pallas_call(
        functools.partial(residual_kernel, count),
        name="residual",
        out_shape=(
            pltpu.VMEM((rows, width), BF),
            pltpu.VMEM((rows, width + LANES), BF),
        ),
        in_specs=[VMEM] * (len(parts) + 2),
        out_specs=(VMEM, VMEM),
        scratch_shapes=[pltpu.VMEM((count, rows, width), BF)],
        compiler_params=pltpu.CompilerParams(vmem_limit_bytes=4 << 20),
        cost_estimate=pl.CostEstimate(flops=10**8, bytes_accessed=1000, transcendentals=0),
    )(*parts, resid, gain)


def tiles(width):
    step = math.gcd(width, TILE)
    return [slice(i, i + step) for i in range(0, width, step)]


def product_kernel(shift, count, cut, *refs):
    block_ref, gate_ref, up_ref, refs = *refs[:3], refs[3:]
    sums, refs = (refs[:2], refs[2:]) if shift else ((), refs)
    step = gate_ref.shape[0]
    at, _ = rows_at(shift, count, step, True)

    def work(gate_out, up_out):
        block = block_ref[:, 0:step]
        for columns in tiles(gate_ref.shape[1]):
            gate_made = jnp.dot(block, gate_ref[:, columns], preferred_element_type=F32)
            up_made = jnp.dot(block, up_ref[at, columns], preferred_element_type=F32)
            gate_out[:, columns] = gate_made + sums[0][:, columns] if sums else gate_made
            up_out[:, columns] = up_made + sums[1][:, columns] if sums else up_made

    if cut is None:
        work(*refs)
        return
    chunk_hbm, gate_out, up_out, chunk_ref, sem = refs
    with_copy(
        [pltpu.make_async_copy(chunk_hbm.at[cut()], chunk_ref, sem)],
        lambda: work(gate_out, up_out),
    )


def product(shift, count, block, gate, up, sums, chunk=None):
    one = pltpu.VMEM((block.shape[0], gate.shape[1]), F32)
    out_shape, scratch_shapes, cut, more = [one, one], [], None, []
    if chunk is not None:
        array, cut, shape = chunk
        more = [pltpu.with_memory_space_constraint(array, pltpu.HBM)]
        out_shape.append(pltpu.VMEM(shape, BF))
        scratch_shapes.append(pltpu.SemaphoreType.DMA)
    return pl.pallas_call(
        functools.partial(product_kernel, shift, count, cut),
        name="product",
        out_shape=tuple(out_shape),
        in_specs=[VMEM] * (3 + len(sums)) + [HBM] * len(more),
        out_specs=tuple([VMEM] * len(out_shape)),
        scratch_shapes=scratch_shapes,
        compiler_params=pltpu.CompilerParams(vmem_limit_bytes=6 << 20),
        cost_estimate=pl.CostEstimate(flops=10**8, bytes_accessed=1000, transcendentals=0),
    )(block, gate, up, *sums, *more)


def routing(ids_ref, logits_ref, mine, rows):
    logits = logits_ref[...]
    first = 1.0 / (1.0 + jnp.exp(logits[1:2, :] - logits[0:1, :]))
    ids = ids_ref[...]
    mix_row = jnp.where(ids[0:1, :] == mine, first, 0.0) + jnp.where(
        ids[1:2, :] == mine, 1.0 - first, 0.0
    )
    eye = lax.broadcasted_iota(jnp.int32, (rows, rows), 0) == lax.broadcasted_iota(
        jnp.int32, (rows, rows), 1
    )
    return jnp.sum(jnp.where(eye, mix_row, 0.0), axis=1, keepdims=True)


def inverse_rms(blocks, width, depth):
    squares = 0.0
    for block in blocks:
        tail = block[:, width:].astype(F32)
        squares = squares + (tail[:, 0:1] + tail[:, 1:2] + tail[:, 2:3])
    return lax.rsqrt(squares / depth + EPSILON)


def activate(gate_sum, up_sum, inverse):
    gate_sum = gate_sum * inverse
    return (gate_sum / (1.0 + jnp.exp(-gate_sum)) * (up_sum * inverse)).astype(BF)


def experts_kernel(count, sharing, last, cut, *refs):
    part_refs, refs = refs[:count], refs[count:]
    ids_ref, logits_ref, gate_ref, up_ref, gate_sum_ref, up_sum_ref, refs = *refs[:6], refs[6:]
    down_refs, down_hbm, refs = refs[: count - 1], refs[count - 1], refs[count:]
    out_refs, refs = refs[:count], refs[count:]
    act, made, mix_ref, last_down, sem = refs
    me = lax.axis_index("expert")
    rows, hidden_units = act.shape
    width = gate_ref.shape[0]
    step = last_down.shape[0]

    def work():
        mix_ref[...] = jnp.broadcast_to(
            routing(ids_ref, logits_ref, me // sharing, rows), mix_ref.shape
        )
        inverse = inverse_rms([ref[...] for ref in part_refs], width, count * width)
        block = part_refs[last][:, 0:width]
        at, _ = rows_at(last, count, width, True)
        for columns in tiles(hidden_units):
            gate_sum = gate_sum_ref[:, columns] + jnp.dot(
                block, gate_ref[:, columns], preferred_element_type=F32
            )
            up_sum = up_sum_ref[:, columns] + jnp.dot(
                block, up_ref[at, columns], preferred_element_type=F32
            )
            act[:, columns] = activate(gate_sum, up_sum, inverse)
        for columns in tiles(count * width):
            made[:, columns] = sum(
                jnp.dot(
                    act[:, c * step : (c + 1) * step], ref[:, columns], preferred_element_type=F32
                )
                for c, ref in enumerate(down_refs)
            )

    with_copy([pltpu.make_async_copy(down_hbm.at[cut()], last_down, sem)], work)
    mix = mix_ref[:, 0:1]
    for shift in range(count):
        at = target(False, count, me, shift)
        columns = pl.ds(pl.multiple_of(at * width, width), width)
        total = made[:, columns] + jnp.dot(
            act[:, hidden_units - step :], last_down[:, columns], preferred_element_type=F32
        )
        out_refs[shift][...] = (total * mix).astype(BF)


def experts(last, parts, ids, logits, gate, up, sums, downs, down_last, count):
    rows, hidden_units = sums[0].shape
    width = gate.shape[0]
    array, cut, shape = down_last
    return pl.pallas_call(
        functools.partial(experts_kernel, count, count // EXPERTS, last, cut),
        name="experts",
        out_shape=tuple([pltpu.VMEM((rows, width), BF)] * count),
        in_specs=[VMEM] * (len(parts) + 6 + len(downs)) + [HBM],
        out_specs=tuple([VMEM] * count),
        scratch_shapes=[
            pltpu.VMEM((rows, hidden_units), BF),
            pltpu.VMEM((rows, count * width), F32),
            pltpu.VMEM((rows, LANES), F32),
            pltpu.VMEM(shape, BF),
            pltpu.SemaphoreType.DMA,
        ],
        compiler_params=pltpu.CompilerParams(vmem_limit_bytes=7 << 20),
        cost_estimate=pl.CostEstimate(flops=10**8, bytes_accessed=1000, transcendentals=0),
    )(
        *parts,
        ids,
        logits,
        gate,
        up,
        *sums,
        *downs,
        pltpu.with_memory_space_constraint(array, pltpu.HBM),
    )


def all_experts_kernel(count, sharing, *refs):
    parts_ref, ids_ref, logits_ref, gate_ref, up_ref, down_ref, out_ref, spread = refs
    depth = gate_ref.shape[0]
    rows = spread.shape[0]
    width = depth // count
    for i in range(count):
        spread[:, i * width : (i + 1) * width] = parts_ref[i, :, 0:width]
    inverse = inverse_rms([parts_ref[i] for i in range(count)], width, depth)
    mix = routing(ids_ref, logits_ref, lax.axis_index("expert") // sharing, rows)
    gate_sum = jnp.dot(spread[...], gate_ref[...], preferred_element_type=F32)
    up_sum = jnp.dot(spread[...], up_ref[...], preferred_element_type=F32)
    act = activate(gate_sum, up_sum, inverse)
    for i in range(count):
        made = jnp.dot(
            act, down_ref[:, i * width : (i + 1) * width], preferred_element_type=F32
        )
        out_ref[i] = (made * mix).astype(BF)


def all_experts(parts, ids, logits, gate, up, down, count):
    rows, depth = ids.shape[1], gate.shape[0]
    return pl.pallas_call(
        functools.partial(all_experts_kernel, count, count // EXPERTS),
        name="experts",
        out_shape=(jax.ShapeDtypeStruct((count, rows, depth // count), BF),),
        in_specs=[VMEM] * 6,
        out_specs=(VMEM,),
        scratch_shapes=[pltpu.VMEM((rows, depth), BF)],
        compiler_params=pltpu.CompilerParams(vmem_limit_bytes=24 << 20),
    )(parts[0], ids, logits, gate, up, down)


def first_sum_kernel(count, other, *refs):
    taken = grouped(count)
    part_refs, out_refs = refs[:taken], refs[taken:]
    me = lax.axis_index("tensor")
    total = sum(piece(part_refs, count, s).astype(F32) for s in range(count))
    rows = total.shape[0] // other
    blocks = [total[i * rows : (i + 1) * rows, :] for i in range(other)]
    for shift in range(other):
        if grouped(other) == 1:
            out_refs[0][shift] = blocks[shift].astype(BF)
        else:
            at = target(False, other, me, shift)
            chosen = sum(jnp.where(at == i, blocks[i], 0.0) for i in range(other))
            out_refs[shift][...] = chosen.astype(BF)


def last_sum_kernel(count, *refs):
    taken = grouped(count)
    part_refs, out_ref = refs[:taken], refs[taken]
    out_ref[...] = sum(piece(part_refs, count, s).astype(F32) for s in range(count)).astype(BF)


def first_sum(parts, count, other, rows, width):
    one = (rows // other, width)
    if grouped(other) == 1:
        out_shape = (jax.ShapeDtypeStruct((other,) + one, BF),)
    else:
        out_shape = tuple([jax.ShapeDtypeStruct(one, BF)] * other)
    return pl.pallas_call(
        functools.partial(first_sum_kernel, count, other),
        name="first_sum",
        out_shape=out_shape,
        in_specs=[VMEM] * len(parts),
        out_specs=tuple([VMEM] * len(out_shape)),
        compiler_params=pltpu.CompilerParams(vmem_limit_bytes=4 << 20),
    )(*parts)


def last_sum(parts, count, shape):
    return pl.pallas_call(
        functools.partial(last_sum_kernel, count),
        name="last_sum",
        out_shape=jax.ShapeDtypeStruct(shape, BF),
        in_specs=[VMEM] * len(parts),
        out_specs=VMEM,
        compiler_params=pltpu.CompilerParams(vmem_limit_bytes=4 << 20),
    )(*parts)


def shards(
    kv_prefill,
    slot_of,
    lengths,
    query,
    new_kv,
    wo,
    resid,
    norm_gain,
    expert_ids,
    gate_logits,
    gate_weight_slabs,
    w_up,
    w_down,
):
    expert_count = lax.axis_size("expert")
    tensor_count = lax.axis_size("tensor")
    total, width = resid.shape
    slots, positions, _, kv_width = kv_prefill.shape
    kv_heads = kv_width // HD
    queries = gather(query, "expert")
    split = len(queries) == expert_count == CHUNKS
    gate, up, down = gate_weight_slabs[0], w_up[0], w_down[0]
    gate_rows = [[rows_of(gate, i, CHUNKS, True)] if split else [] for i in range(CHUNKS)]
    down_rows = [[rows_of(down, i, CHUNKS, False)] if split else [] for i in range(CHUNKS)]
    head_shape = (slots, positions, 2, HD)
    heads = [
        (kv_prefill, (slice(None), slice(None), slice(None), pl.ds(g * HD, HD)), head_shape)
        for g in range(kv_heads)
    ]
    own, fresh, *loaded = load(
        [whole(query), whole(new_kv), *heads, *gate_rows[0], *gate_rows[3]]
    )
    caches, first_gates = loaded[:kv_heads], loaded[kv_heads:]
    if split:
        queries[0] = own
    caches = [cache.reshape(slots, 2 * positions, HD) for cache in caches]
    part, *second_gates = attend(
        slot_of,
        lengths,
        queries,
        fresh,
        caches,
        gate_rows[2][0] if split else None,
        expert_count,
    )
    parts = gather(part, "expert")
    wo_here, resid_here, gain_here, *third = load(
        [whole(wo), whole(resid), whole(norm_gain), *gate_rows[1], *down_rows[0]], [part]
    )
    projected = project(parts, wo_here, expert_count, total)
    partials = gather(projected, "tensor")
    attention, scaled = residual(partials, resid_here, gain_here, tensor_count)
    blocks = gather(scaled, "expert")
    if split:
        g_0, g_3, g_2, g_1, d_0 = *first_gates, *second_gates, *third
        *sums, d_1 = product(0, CHUNKS, blocks[0], g_0, up, (), down_rows[1][0])
        *sums, d_2 = product(3, CHUNKS, blocks[3], g_3, up, sums, down_rows[2][0])
        sums = product(2, CHUNKS, blocks[2], g_2, up, sums)
        outgoing = experts(
            1,
            blocks,
            expert_ids.T,
            gate_logits.T,
            g_1,
            up,
            sums,
            (d_0, d_1, d_2),
            down_rows[3][0],
            CHUNKS,
        )
    else:
        outgoing = all_experts(
            blocks, expert_ids.T, gate_logits.T, gate, up, down, expert_count
        )
    column_parts = first_sum(
        exchange(outgoing, "expert"), expert_count, tensor_count, total, width
    )
    moe_out = last_sum(
        exchange(column_parts, "tensor"), tensor_count, (total // tensor_count, width)
    )
    return (attention, moe_out)


def solution(mesh):
    return jax.shard_map(
        shards,
        mesh=mesh,
        in_specs=(
            P("groups", "expert", None, "tensor"),
            P("groups"),
            P("groups"),
            P(("groups", "expert"), "tensor"),
            P(("groups", "expert"), None, "tensor"),
            P("tensor", "expert"),
            P("groups", "expert"),
            P("expert"),
            P("groups", None),
            P("groups", None),
            P("expert", None, "tensor"),
            P("expert", None, "tensor"),
            P("expert", "tensor", None),
        ),
        out_specs=(P("groups", "expert"), P(("groups", "tensor"), "expert")),
        check_vma=False,
    )
```

```python
import functools
import math

import jax
import jax.numpy as jnp
from jax import lax
from jax.experimental import pallas as pl
from jax.experimental.pallas import tpu as pltpu
from jax.sharding import PartitionSpec as P

HEADS = 32
KVH = 8
HD = 128
EXPERTS = 4
EPSILON = 1e-05
MASKED = -1e30
LIVE = -1e29
LANES = 128
STATS = 16
MOST_PERMUTES = 4
CHUNKS = 4
TILE = 512
EXPERTS_MIB = 4

BF = jnp.bfloat16
F32 = jnp.float32
VMEM = pl.BlockSpec(memory_space=pltpu.VMEM)
SMEM = pl.BlockSpec(memory_space=pltpu.SMEM)
HBM = pl.BlockSpec(memory_space=pltpu.HBM)


def gather(value, axis):
    count = lax.axis_size(axis)
    if count > MOST_PERMUTES:
        return [lax.all_gather(value, axis)]
    out = [value]
    for shift in range(1, count):
        out.append(lax.ppermute(value, axis, [(i, (i + shift) % count) for i in range(count)]))
    return out


def exchange(values, axis):
    count = lax.axis_size(axis)
    if count > MOST_PERMUTES:
        return [lax.all_to_all(values[0], axis, 0, 0, tiled=True)]
    out = [values[0]]
    for shift in range(1, count):
        out.append(
            lax.ppermute(values[shift], axis, [(i, (i + shift) % count) for i in range(count)])
        )
    return out


def piece(refs, count, shift):
    return refs[shift][...] if len(refs) == count else refs[0][shift]


def source(refs, count, me, shift):
    return lax.rem(me - shift + count, count) if len(refs) == count else shift


def target(stacked, count, me, shift):
    return shift if stacked else lax.rem(me + shift, count)


def grouped(count):
    return 1 if count > MOST_PERMUTES else count


def load_kernel(cuts, waits, *refs):
    count = len(cuts)
    sources, outs, sems = refs[:count], refs[count + waits : -1], refs[-1]
    copies = []
    for i, cut in enumerate(cuts):
        view = sources[i] if cut is None else sources[i].at[cut() if callable(cut) else cut]
        copies.append(pltpu.make_async_copy(view, outs[i], sems.at[i]))
    for copy in copies:
        copy.start()
    for copy in copies:
        copy.wait()


def load(items, waits=(), flops=10**8):
    hbm = lambda w: pltpu.with_memory_space_constraint(w, pltpu.HBM)
    return pl.pallas_call(
        functools.partial(load_kernel, [cut for _, cut, _ in items], len(waits)),
        name="load",
        out_shape=tuple(pltpu.VMEM(shape, array.dtype) for array, _, shape in items),
        in_specs=[HBM] * len(items) + [pl.BlockSpec(memory_space=pl.ANY)] * len(waits),
        out_specs=tuple([VMEM] * len(items)),
        scratch_shapes=[pltpu.SemaphoreType.DMA((len(items),))],
        compiler_params=pltpu.CompilerParams(vmem_limit_bytes=1 << 20),
        cost_estimate=pl.CostEstimate(flops=flops, bytes_accessed=1000, transcendentals=0),
    )(*[hbm(array) for array, _, _ in items], *waits)


def whole(array):
    return (array, None, array.shape)


def rows_at(part, count, step, relative):
    if relative:
        part = lax.rem(lax.axis_index("expert") - part + count, count)
        return (pl.ds(pl.multiple_of(part * step, step), step), slice(None))
    return (pl.ds(part * step, step), slice(None))


def rows_of(array, part, count, relative):
    step = array.shape[0] // count
    cut = functools.partial(rows_at, part, count, step, relative)
    return (array, cut, (step, array.shape[1]))


def attend_kernel(count, own_rows, kv_heads, group, positions, *refs):
    taken = grouped(count)
    slot_ref, length_ref = refs[0], refs[1]
    query_refs = refs[2 : 2 + taken]
    new_ref = refs[2 + taken]
    cache_refs = refs[3 + taken : 3 + taken + kv_heads]
    out_ref, q_rows, score, acc, fresh = refs[3 + taken + kv_heads :]
    me = lax.axis_index("expert")
    heads = kv_heads * group
    total = count * own_rows
    rows = total * heads
    width = 2 * positions
    scale = 1.0 / math.sqrt(HD)
    for shift in range(count):
        block = piece(query_refs, count, shift).astype(F32)
        where_to = source(query_refs, count, me, shift)
        for head in range(heads):
            q_rows[where_to, pl.ds(head, own_rows, stride=heads), :] = block[
                :, head * HD : (head + 1) * HD
            ]
    head_of_row = lax.broadcasted_iota(jnp.int32, (heads, HD), 0) // group
    lane = lax.broadcasted_iota(jnp.int32, (heads, width), 1)
    position = me * positions + lane // 2
    is_key = lax.rem(lane, 2) == 0

    def cached(b):
        at = slot_ref[b]
        return jnp.concatenate([ref[at] for ref in cache_refs], axis=1)

    def diagonal(parts):
        return sum(jnp.where(head_of_row == g, parts(g), 0.0) for g in range(kv_heads))

    def scores(b):
        owner, within = b // own_rows, lax.rem(b, own_rows)
        vectors = q_rows[owner, pl.ds(pl.multiple_of(within * heads, heads), heads), :]
        spread = jnp.concatenate(
            [jnp.where(head_of_row == g, vectors, 0.0) for g in range(kv_heads)], axis=1
        ).astype(BF)
        both = cached(b)
        found = (
            lax.dot_general(
                spread, both, (((1,), (1,)), ((), ())), preferred_element_type=F32
            )
            * scale
        )
        live = is_key & (position < length_ref[b])
        score[pl.ds(pl.multiple_of(b * heads, heads), heads), :] = jnp.where(live, found, MASKED)

    def values(b):
        at = pl.ds(pl.multiple_of(b * heads, heads), heads)
        both = cached(b)
        summed = jnp.dot(score[at, :].astype(BF), both, preferred_element_type=F32)
        acc[at, :] = diagonal(lambda g: summed[:, g * HD : (g + 1) * HD])

    def sweep(step):
        if total <= 16:
            for b in range(total):
                step(b)
        else:
            pl.loop(0, total)(step)

    sweep(scores)
    own = own_rows * heads
    new = new_ref[...].astype(F32)
    for b in range(own_rows):
        for g in range(kv_heads):
            at = b * heads + g * group
            for which in range(2):
                fresh[which, at : at + group, :] = jnp.broadcast_to(
                    new[b, which : which + 1, g * HD : (g + 1) * HD], (group, HD)
                )
    own_score = jnp.sum(q_rows[me] * fresh[0], axis=1, keepdims=True) * scale
    row = lax.broadcasted_iota(jnp.int32, (rows, 1), 0)
    at_home = (row >= me * own) & (row < (me + 1) * own)
    own_all = jnp.concatenate([own_score] * count, axis=0)
    own_all = jnp.where(at_home, own_all, MASKED)
    raw = score[...]
    peak = jnp.maximum(jnp.max(raw, axis=1, keepdims=True), own_all).astype(BF).astype(F32)
    weights = jnp.where(raw > LIVE, jnp.exp(raw - peak), 0.0)
    own_weight = jnp.where(at_home, jnp.exp(own_all - peak), 0.0)
    weight_sum = jnp.sum(weights, axis=1, keepdims=True) + own_weight
    score[...] = pltpu.roll(weights, 1, 1)
    sweep(values)
    fresh_all = jnp.concatenate([fresh[1]] * count, axis=0)
    out_ref[0:rows, :] = (acc[...] + own_weight * fresh_all).astype(BF)
    high = weight_sum.astype(BF).astype(F32)
    low = weight_sum - high
    column = lax.broadcasted_iota(jnp.int32, (rows, LANES), 1)
    table = jnp.where(
        column == 0, peak, jnp.where(column == 1, high, jnp.where(column == 2, low, 0.0))
    )
    for part in range(rows // LANES):
        turned = table[part * LANES : (part + 1) * LANES, :].T
        out_ref[rows + part * STATS : rows + (part + 1) * STATS, :] = turned[0:STATS, :].astype(BF)


def attend(slot_of, lengths, queries, new_kv, caches, count):
    own_rows, _, kv_width = new_kv.shape
    kv_heads = kv_width // HD
    group = HEADS // KVH
    heads = kv_heads * group
    positions = caches[0].shape[1] // 2
    rows = count * own_rows * heads
    return pl.pallas_call(
        functools.partial(attend_kernel, count, own_rows, kv_heads, group, positions),
        name="attend",
        out_shape=pltpu.VMEM((rows + STATS * (rows // LANES), LANES), BF),
        in_specs=[SMEM, SMEM] + [VMEM] * (len(queries) + 1 + kv_heads),
        out_specs=VMEM,
        scratch_shapes=[
            pltpu.VMEM((count, own_rows * heads, HD), F32),
            pltpu.VMEM((rows, 2 * positions), F32),
            pltpu.VMEM((rows, HD), F32),
            pltpu.VMEM((2, own_rows * heads, HD), F32),
        ],
        compiler_params=pltpu.CompilerParams(vmem_limit_bytes=6 << 20),
        cost_estimate=pl.CostEstimate(flops=10**8, bytes_accessed=1000, transcendentals=0),
    )(slot_of, lengths, *queries, new_kv, *caches)


def project_kernel(count, rows, heads, *refs):
    taken = grouped(count)
    part_refs = refs[:taken]
    wo_ref, out_ref, joined, context = refs[taken:]
    parts = [piece(part_refs, count, s) for s in range(count)]

    def stats(part):
        tables = []
        for block in range(rows // LANES):
            at = rows + block * STATS
            table = part[at : at + STATS, :].astype(F32)
            tall = jnp.concatenate([table, jnp.zeros((LANES - STATS, LANES), F32)], axis=0)
            tables.append(tall.T)
        table = jnp.concatenate(tables, axis=0)
        return table[:, 0:1], table[:, 1:2] + table[:, 2:3]

    found = [stats(part) for part in parts]
    peak = functools.reduce(jnp.maximum, [m for m, _ in found])
    weights = [jnp.exp(m - peak) for m, _ in found]
    denominator = sum(w * l for w, (_, l) in zip(weights, found))
    numerator = sum(w * part[0:rows, :].astype(F32) for w, part in zip(weights, parts))
    joined[...] = numerator / denominator
    total = rows // heads
    for head in range(heads):
        context[:, head * HD : (head + 1) * HD] = joined[
            pl.ds(head, total, stride=heads), :
        ].astype(BF)
    out_ref[...] = jnp.dot(context[...], wo_ref[...], preferred_element_type=F32).astype(BF)


def project(parts, wo, count, total):
    heads = wo.shape[0] // HD
    rows = total * heads
    return pl.pallas_call(
        functools.partial(project_kernel, count, rows, heads),
        name="project",
        out_shape=jax.ShapeDtypeStruct((total, wo.shape[1]), BF),
        in_specs=[VMEM] * (len(parts) + 1),
        out_specs=VMEM,
        scratch_shapes=[
            pltpu.VMEM((rows, HD), F32),
            pltpu.VMEM((total, wo.shape[0]), BF),
        ],
        compiler_params=pltpu.CompilerParams(vmem_limit_bytes=(4 if len(parts) == count else 48) << 20),
        cost_estimate=pl.CostEstimate(flops=10**11, bytes_accessed=1000, transcendentals=0),
    )(*parts, wo)


def residual_kernel(count, *refs):
    taken = grouped(count)
    part_refs = refs[:taken]
    resid_ref, gain_ref, attn_ref, out_ref, ordered = refs[taken:]
    me = lax.axis_index("tensor")
    for shift in range(count):
        ordered[source(part_refs, count, me, shift)] = piece(part_refs, count, shift)
    attention = sum(ordered[i].astype(F32) for i in range(count)).astype(BF)
    attn_ref[...] = attention
    hidden = resid_ref[...].astype(F32) + attention.astype(F32)
    squares = jnp.sum(hidden * hidden, axis=1, keepdims=True)
    width = hidden.shape[1]
    gain = gain_ref[...].astype(F32).reshape(1, width)
    out_ref[:, 0:width] = (hidden * gain).astype(BF)
    high = squares.astype(BF).astype(F32)
    middle = (squares - high).astype(BF).astype(F32)
    low = squares - high - middle
    column = lax.broadcasted_iota(jnp.int32, (hidden.shape[0], LANES), 1)
    out_ref[:, width:] = jnp.where(
        column == 0, high, jnp.where(column == 1, middle, jnp.where(column == 2, low, 0.0))
    ).astype(BF)


def residual(parts, resid, gain, count):
    rows, width = resid.shape
    return pl.pallas_call(
        functools.partial(residual_kernel, count),
        name="residual",
        out_shape=(
            pltpu.VMEM((rows, width), BF),
            pltpu.VMEM((rows, width + LANES), BF),
        ),
        in_specs=[VMEM] * (len(parts) + 2),
        out_specs=(VMEM, VMEM),
        scratch_shapes=[pltpu.VMEM((count, rows, width), BF)],
        compiler_params=pltpu.CompilerParams(vmem_limit_bytes=4 << 20),
        cost_estimate=pl.CostEstimate(flops=10**8, bytes_accessed=1000, transcendentals=0),
    )(*parts, resid, gain)


def tiles(width):
    step = math.gcd(width, TILE)
    return [slice(i, i + step) for i in range(0, width, step)]


def product_kernel(block_ref, gate_ref, *refs):
    before, out_ref = refs[:-1], refs[-1]
    block = block_ref[:, 0 : gate_ref.shape[0]]
    for columns in tiles(gate_ref.shape[1]):
        made = jnp.dot(block, gate_ref[:, columns], preferred_element_type=F32)
        out_ref[:, columns] = made + before[0][:, columns] if before else made


def product(block, gate, before):
    return pl.pallas_call(
        product_kernel,
        name="product",
        out_shape=pltpu.VMEM((block.shape[0], gate.shape[1]), F32),
        in_specs=[VMEM] * (2 + len(before)),
        out_specs=VMEM,
        compiler_params=pltpu.CompilerParams(vmem_limit_bytes=2 << 20),
        cost_estimate=pl.CostEstimate(flops=10**8, bytes_accessed=1000, transcendentals=0),
    )(block, gate, *before)


def routing(ids_ref, logits_ref, mine, rows):
    logits = logits_ref[...]
    first = 1.0 / (1.0 + jnp.exp(logits[1:2, :] - logits[0:1, :]))
    ids = ids_ref[...]
    mix_row = jnp.where(ids[0:1, :] == mine, first, 0.0) + jnp.where(
        ids[1:2, :] == mine, 1.0 - first, 0.0
    )
    eye = lax.broadcasted_iota(jnp.int32, (rows, rows), 0) == lax.broadcasted_iota(
        jnp.int32, (rows, rows), 1
    )
    return jnp.sum(jnp.where(eye, mix_row, 0.0), axis=1, keepdims=True)


def inverse_rms(blocks, width, depth):
    squares = 0.0
    for block in blocks:
        tail = block[:, width:].astype(F32)
        squares = squares + (tail[:, 0:1] + tail[:, 1:2] + tail[:, 2:3])
    return lax.rsqrt(squares / depth + EPSILON)


def activate(gate_sum, up_sum, inverse):
    gate_sum = gate_sum * inverse
    return (gate_sum / (1.0 + jnp.exp(-gate_sum)) * (up_sum * inverse)).astype(BF)


def experts_kernel(count, holders, sharing, last, *refs):
    part_refs, refs = refs[:count], refs[count:]
    ids_ref, logits_ref, gate_ref, sum_ref, up_ref, down_ref, *out_refs = refs
    *out_refs, spread, act, made = out_refs
    me = lax.axis_index("expert")
    rows, depth = spread.shape
    width = depth // count
    for shift in range(count):
        at = source(part_refs, count, me, shift)
        spread[:, pl.ds(pl.multiple_of(at * width, width), width)] = part_refs[shift][:, 0:width]
    mix = routing(ids_ref, logits_ref, me // sharing, rows)
    inverse = inverse_rms([ref[...] for ref in part_refs], width, depth)
    block = part_refs[last][:, 0:width]
    for columns in tiles(act.shape[1]):
        gate_sum = sum_ref[:, columns] + jnp.dot(
            block, gate_ref[:, columns], preferred_element_type=F32
        )
        up_sum = jnp.dot(spread[...], up_ref[:, columns], preferred_element_type=F32)
        act[:, columns] = activate(gate_sum, up_sum, inverse)
    for columns in tiles(depth):
        made[:, columns] = mix * jnp.dot(
            act[...], down_ref[:, columns], preferred_element_type=F32
        )
    own = rows // holders
    mine = lax.axis_index("tensor")
    for shift in range(holders):
        at = target(False, holders, mine, shift)
        chosen = sum(
            jnp.where(at == i, made[i * own : (i + 1) * own, :], 0.0) for i in range(holders)
        )
        out_refs[shift][...] = chosen.astype(BF)


def experts(last, parts, ids, logits, gate, gate_sum, up, down, count, holders):
    rows, (hidden_units, depth) = gate_sum.shape[0], down.shape
    return pl.pallas_call(
        functools.partial(experts_kernel, count, holders, count // EXPERTS, last),
        name="experts",
        out_shape=tuple([pltpu.VMEM((rows // holders, depth), BF)] * holders),
        in_specs=[VMEM] * (len(parts) + 6),
        out_specs=tuple([VMEM] * holders),
        scratch_shapes=[
            pltpu.VMEM((rows, depth), BF),
            pltpu.VMEM((rows, hidden_units), BF),
            pltpu.VMEM((rows, depth), F32),
        ],
        compiler_params=pltpu.CompilerParams(vmem_limit_bytes=EXPERTS_MIB << 20),
        cost_estimate=pl.CostEstimate(flops=10**8, bytes_accessed=1000, transcendentals=0),
    )(*parts, ids, logits, gate, gate_sum, up, down)


def all_experts_kernel(count, sharing, *refs):
    parts_ref, ids_ref, logits_ref, gate_ref, up_ref, down_ref, out_ref, spread = refs
    depth = gate_ref.shape[0]
    rows = spread.shape[0]
    width = depth // count
    for i in range(count):
        spread[:, i * width : (i + 1) * width] = parts_ref[i, :, 0:width]
    inverse = inverse_rms([parts_ref[i] for i in range(count)], width, depth)
    mix = routing(ids_ref, logits_ref, lax.axis_index("expert") // sharing, rows)
    gate_sum = jnp.dot(spread[...], gate_ref[...], preferred_element_type=F32)
    up_sum = jnp.dot(spread[...], up_ref[...], preferred_element_type=F32)
    act = activate(gate_sum, up_sum, inverse)
    for i in range(count):
        made = jnp.dot(
            act, down_ref[:, i * width : (i + 1) * width], preferred_element_type=F32
        )
        out_ref[i] = (made * mix).astype(BF)


def all_experts(parts, ids, logits, gate, up, down, count):
    rows, depth = ids.shape[1], gate.shape[0]
    return pl.pallas_call(
        functools.partial(all_experts_kernel, count, count // EXPERTS),
        name="experts",
        out_shape=(jax.ShapeDtypeStruct((count, rows, depth // count), BF),),
        in_specs=[VMEM] * 6,
        out_specs=(VMEM,),
        scratch_shapes=[pltpu.VMEM((rows, depth), BF)],
        compiler_params=pltpu.CompilerParams(vmem_limit_bytes=24 << 20),
    )(parts[0], ids, logits, gate, up, down)


def first_sum_kernel(count, other, *refs):
    taken = grouped(count)
    part_refs, out_refs = refs[:taken], refs[taken:]
    me = lax.axis_index("tensor")
    total = sum(piece(part_refs, count, s).astype(F32) for s in range(count))
    rows = total.shape[0] // other
    blocks = [total[i * rows : (i + 1) * rows, :] for i in range(other)]
    for shift in range(other):
        if grouped(other) == 1:
            out_refs[0][shift] = blocks[shift].astype(BF)
        else:
            at = target(False, other, me, shift)
            chosen = sum(jnp.where(at == i, blocks[i], 0.0) for i in range(other))
            out_refs[shift][...] = chosen.astype(BF)


def token_sum_kernel(count, other, *refs):
    part_refs, out_refs, total = refs[:count], refs[count:-1], refs[-1]
    me = lax.axis_index("expert")
    total[...] = sum(ref[...].astype(F32) for ref in part_refs)
    width = total.shape[1] // other
    for shift in range(other):
        at = target(False, other, me, shift)
        columns = pl.ds(pl.multiple_of(at * width, width), width)
        out_refs[shift][...] = total[:, columns].astype(BF)


def token_sum(parts, count, other):
    rows, depth = parts[0].shape
    return pl.pallas_call(
        functools.partial(token_sum_kernel, count, other),
        name="first_sum",
        out_shape=tuple([pltpu.VMEM((rows, depth // other), BF)] * other),
        in_specs=[VMEM] * count,
        out_specs=tuple([VMEM] * other),
        scratch_shapes=[pltpu.VMEM((rows, depth), F32)],
        compiler_params=pltpu.CompilerParams(vmem_limit_bytes=2 << 20),
    )(*parts)


def last_sum_kernel(count, *refs):
    taken = grouped(count)
    part_refs, out_ref = refs[:taken], refs[taken]
    out_ref[...] = sum(piece(part_refs, count, s).astype(F32) for s in range(count)).astype(BF)


def first_sum(parts, count, other, rows, width):
    one = (rows // other, width)
    if grouped(other) == 1:
        out_shape = (jax.ShapeDtypeStruct((other,) + one, BF),)
    else:
        out_shape = tuple([jax.ShapeDtypeStruct(one, BF)] * other)
    return pl.pallas_call(
        functools.partial(first_sum_kernel, count, other),
        name="first_sum",
        out_shape=out_shape,
        in_specs=[VMEM] * len(parts),
        out_specs=tuple([VMEM] * len(out_shape)),
        compiler_params=pltpu.CompilerParams(vmem_limit_bytes=4 << 20),
    )(*parts)


def last_sum(parts, count, shape):
    return pl.pallas_call(
        functools.partial(last_sum_kernel, count),
        name="last_sum",
        out_shape=jax.ShapeDtypeStruct(shape, BF),
        in_specs=[VMEM] * len(parts),
        out_specs=VMEM,
        compiler_params=pltpu.CompilerParams(vmem_limit_bytes=4 << 20),
    )(*parts)


def shards(
    kv_prefill,
    slot_of,
    lengths,
    query,
    new_kv,
    wo,
    resid,
    norm_gain,
    expert_ids,
    gate_logits,
    gate_weight_slabs,
    w_up,
    w_down,
):
    expert_count = lax.axis_size("expert")
    tensor_count = lax.axis_size("tensor")
    total, width = resid.shape
    slots, positions, _, kv_width = kv_prefill.shape
    kv_heads = kv_width // HD
    queries = gather(query, "expert")
    split = len(queries) == expert_count == CHUNKS
    gate, up, down = gate_weight_slabs[0], w_up[0], w_down[0]
    gate_rows = [[rows_of(gate, i, CHUNKS, True)] if split else [] for i in range(CHUNKS)]
    head_shape = (slots, positions, 2, HD)
    heads = [
        (kv_prefill, (slice(None), slice(None), slice(None), pl.ds(g * HD, HD)), head_shape)
        for g in range(kv_heads)
    ]
    own, fresh, *loaded = load(
        [whole(query), whole(new_kv), *heads, *gate_rows[0], *gate_rows[3]]
    )
    caches, first_gates = loaded[:kv_heads], loaded[kv_heads:]
    if split:
        queries[0] = own
    caches = [cache.reshape(slots, 2 * positions, HD) for cache in caches]
    part = attend(
        slot_of,
        lengths,
        queries,
        fresh,
        caches,
        expert_count,
    )
    parts = gather(part, "expert")
    wo_here, resid_here, gain_here, *third = load(
        [whole(wo), whole(resid), whole(norm_gain), *gate_rows[2], *gate_rows[1]], [part]
    )
    projected = project(parts, wo_here, expert_count, total)
    partials = gather(projected, "tensor")
    attention, scaled = residual(partials, resid_here, gain_here, tensor_count)
    blocks = gather(scaled, "expert")
    if split:
        g_0, g_3, g_2, g_1 = *first_gates, *third
        gate_sum = product(blocks[0], g_0, ())
        gate_sum = product(blocks[3], g_3, (gate_sum,))
        gate_sum = product(blocks[2], g_2, (gate_sum,))
        outgoing = experts(
            1,
            blocks,
            expert_ids.T,
            gate_logits.T,
            g_1,
            gate_sum,
            up,
            down,
            CHUNKS,
            tensor_count,
        )
        token_parts = token_sum(
            exchange(outgoing, "tensor"), tensor_count, expert_count
        )
        moe_out = last_sum(
            exchange(token_parts, "expert"), expert_count, (total // tensor_count, width)
        )
    else:
        outgoing = all_experts(
            blocks, expert_ids.T, gate_logits.T, gate, up, down, expert_count
        )
        column_parts = first_sum(
            exchange(outgoing, "expert"), expert_count, tensor_count, total, width
        )
        moe_out = last_sum(
            exchange(column_parts, "tensor"), tensor_count, (total // tensor_count, width)
        )
    return (attention, moe_out)


def solution(mesh):
    return jax.shard_map(
        shards,
        mesh=mesh,
        in_specs=(
            P("groups", "expert", None, "tensor"),
            P("groups"),
            P("groups"),
            P(("groups", "expert"), "tensor"),
            P(("groups", "expert"), None, "tensor"),
            P("tensor", "expert"),
            P("groups", "expert"),
            P("expert"),
            P("groups", None),
            P("groups", None),
            P("expert", None, "tensor"),
            P("expert", None, "tensor"),
            P("expert", "tensor", None),
        ),
        out_specs=(P("groups", "expert"), P(("groups", "tensor"), "expert")),
        check_vma=False,
    )
```
